32 devices in a mesh: wa: 4 (over z), bl: 8 (over y, x, core).
Axes of the slice: x: 2, y: 2, z: 4, core: 2. Of those that a mesh axis runs over, the one named last changes fastest.
Arguments:
- visibilities: float32 [4, 16, 2, 128], P('wa', 'bl'), may hold values from -6 to 6
- weights: float32 [4, 16, 128], P('wa', 'bl'), may hold values from 0.25 to 4
- cell_index: int32 [4, 16, 128], P('wa', 'bl'), may hold values from 0 to 1048575
- kernel_index: int32 [4, 16, 128], P('wa', 'bl'), may hold values from 0 to 255
- layer_index: int32 [4, 16, 128], P('wa', 'bl'), may hold values from 0 to 1
- tile_counts: int32 [4, 16], P('wa', 'bl'), may hold values from 1 to 128
- kernel_table: float32 [16, 8], replicated, may hold values from 0.05 to 0.3
- layer_depth: float32 [8], P('wa'), may hold values from -150 to 150
Outputs:
- image: float32 [1024, 1024], P('wa', 'bl')
The draws below stay inside these ranges and needn't reach their ends.
All inputs are finite; a program needn't handle non-finite values.
Results may differ from the reference program's by a relative error of at most 0.0003.
Values sent between devices are 32-bit elements; how exact they have to be, the bound alone decides.
A program may use at most 128 MiB of HBM per device.

```python
import math
import jax
import jax.numpy as jnp
from jax import lax

GRID = 1024
SUPPORT = 8
OVERSAMPLE = 16
SAMPLES = 128
LAYER_DEV = 2
WGROUPS = 4
LAYERS = 8
TILES = 16


def place_ends(drawn, key, least, top_value):
    extent = drawn.shape
    place = [jax.random.randint(jax.random.fold_in(key, axis), (), 0, extent[axis]) for axis in range(len(extent))]
    drawn = drawn.at[tuple(place)].set(least)
    longest = extent.index(max(extent))
    place[longest] = (place[longest] + 1) % extent[longest]
    return drawn.at[tuple(place)].set(top_value)


def block_scale(own_key, dims, pieces, low, largest):
    def one(dim, parts):
        draws = jax.random.uniform(jax.random.fold_in(jax.random.fold_in(own_key, 6), dim), (parts,), jnp.float32, low / len(pieces), largest / len(pieces))
        return jnp.repeat(jnp.exp(draws), dims[dim] // parts).reshape((-1,) + (1,) * (len(dims) - dim - 1))

    gain = one(*pieces[0])
    for cut in pieces[1:]:
        gain = gain * one(*cut)
    return gain


def scatter_about(key, shape, spread, bound, split=(), kind=jnp.bfloat16):
    loudness = block_scale(key, shape, split, -0.22, 0.18) if split else 1.0
    array = jax.random.normal(key, shape, jnp.float32) * spread * loudness
    return jnp.minimum(jnp.maximum(array, -bound), bound).astype(kind)


def setup_inputs(seed: int = 0) -> dict:
    seeds = jax.random.split(jax.random.key(seed), 9)
    visibilities = scatter_about(seeds[0], (WGROUPS, TILES, 2, SAMPLES), 1.0, 6.0, ((0, 4), (1, 8)), jnp.float32)
    weights = jnp.clip(jnp.exp(math.log(4.0) - 2.7725887 * jax.random.uniform(seeds[1], (WGROUPS, TILES, SAMPLES), jnp.float32) ** block_scale(seeds[1], (WGROUPS, TILES, SAMPLES), ((0, 4), (1, 8)), -0.2, 0.2)), 0.25, 4.0)
    cell_index = place_ends(jax.random.randint(seeds[2], (WGROUPS, TILES, SAMPLES), 0, GRID * GRID), jax.random.fold_in(seeds[2], 1), 0, (GRID * GRID) - 1).astype(jnp.int32)
    kernel_index = place_ends(jax.random.randint(seeds[3], (WGROUPS, TILES, SAMPLES), 0, OVERSAMPLE * OVERSAMPLE), jax.random.fold_in(seeds[3], 1), 0, (OVERSAMPLE * OVERSAMPLE) - 1).astype(jnp.int32)
    layer_index = place_ends(jax.random.randint(seeds[4], (WGROUPS, TILES, SAMPLES), 0, LAYER_DEV), jax.random.fold_in(seeds[4], 1), 0, LAYER_DEV - 1).astype(jnp.int32)
    tile_counts = place_ends(jax.random.randint(seeds[5], (WGROUPS, TILES), 1, SAMPLES + 1), jax.random.fold_in(seeds[5], 1), 1, SAMPLES).astype(jnp.int32)
    kernel_table = jnp.clip(jax.random.uniform(seeds[6], (OVERSAMPLE, SUPPORT), jnp.float32, 0.05, 0.3), 0.05, 0.3)
    layer_depth = jnp.clip(jax.random.uniform(seeds[7], (LAYERS,), jnp.float32, -150.0, 150.0) * block_scale(seeds[7], (LAYERS,), ((0, 4),), -0.4, 0.0), -150.0, 150.0)
    return dict(visibilities=visibilities, weights=weights, cell_index=cell_index, kernel_index=kernel_index, layer_index=layer_index, tile_counts=tile_counts, kernel_table=kernel_table, layer_depth=layer_depth)


field_of_view = 0.6

def reference(visibilities, weights, cell_index, kernel_index, layer_index, tile_counts, kernel_table, layer_depth):
    position = lax.broadcasted_iota(jnp.int32, cell_index.shape, 2)
    usable = position < tile_counts[:, :, None]
    used_weight = jnp.where(usable, weights, jnp.float32(0.0))
    square_sum = jnp.sum(used_weight * used_weight)
    group_index = lax.broadcasted_iota(jnp.int32, cell_index.shape, 0)
    global_layer = group_index * LAYER_DEV + layer_index
    row_cell = cell_index // GRID
    col_cell = cell_index % GRID
    row_kernel = kernel_table[kernel_index // OVERSAMPLE]
    col_kernel = kernel_table[kernel_index % OVERSAMPLE]
    offsets = jnp.arange(SUPPORT, dtype=jnp.int32) - SUPPORT // 2
    row_target = (row_cell[..., None] + offsets) % GRID
    col_target = (col_cell[..., None] + offsets) % GRID
    amount = row_kernel[..., :, None] * col_kernel[..., None, :]
    vis_real = visibilities[:, :, 0, :] * used_weight
    vis_imag = visibilities[:, :, 1, :] * used_weight
    layer_cells = global_layer[..., None, None]
    row_cells = row_target[..., :, None]
    col_cells = col_target[..., None, :]
    grid_real = jnp.zeros((LAYERS, GRID, GRID), jnp.float32).at[layer_cells, row_cells, col_cells].add(vis_real[..., None, None] * amount)
    grid_imag = jnp.zeros((LAYERS, GRID, GRID), jnp.float32).at[layer_cells, row_cells, col_cells].add(vis_imag[..., None, None] * amount)
    coords = (jnp.arange(GRID, dtype=jnp.int32) - GRID // 2).astype(jnp.float32) * (field_of_view / GRID)
    depth_term = jnp.sqrt(1.0 - coords[:, None] * coords[:, None] - coords[None, :] * coords[None, :]) - 1.0

    def add_layer(accumulated, layer_item):
        part_real, part_imag, depth_value = layer_item
        spectrum = jnp.fft.ifft2(part_real + 1j * part_imag) * (GRID * GRID)
        phases = 2.0 * jnp.pi * depth_value * depth_term
        return (accumulated + (jnp.real(spectrum) * jnp.cos(phases) - jnp.imag(spectrum) * jnp.sin(phases)), None)
    screened, unused = lax.scan(add_layer, jnp.zeros((GRID, GRID), jnp.float32), (grid_real, grid_imag, layer_depth))
    return screened / jnp.sqrt(square_sum)
```

```python
import functools
import math

import jax
import jax.numpy as jnp
from jax import lax
from jax.experimental import pallas as pl
from jax.experimental.pallas import tpu as pltpu
from jax.sharding import PartitionSpec as P

GRID = 1024
SUPPORT = 8
OVERSAMPLE = 16
LANES = 128
FINE = 32
XBLOCK = 128

field_of_view = 0.6
MESH = pl.DeviceIdType.MESH

TWO_PI = 2.0 * math.pi
SIN_TERMS = [(-1) ** k * TWO_PI ** (2 * k + 1) / math.factorial(2 * k + 1) for k in range(9)]
COS_TERMS = [(-1) ** k * TWO_PI ** (2 * k) / math.factorial(2 * k) for k in range(10)]


def horner(square, terms):
    value = jnp.full_like(square, terms[-1])
    for term in terms[-2::-1]:
        value = value * square + term
    return value


def turn_cos_sin(turns):
    part = turns - jnp.round(turns)
    square = part * part
    return horner(square, COS_TERMS), part * horner(square, SIN_TERMS)


def split(value):
    high = value.astype(jnp.bfloat16)
    return high, (value - high.astype(jnp.float32)).astype(jnp.bfloat16)


def dot_nt(a, b):
    return lax.dot_general(
        a, b, (((1,), (1,)), ((), ())), preferred_element_type=jnp.float32
    )


def greet(axis, me, count):
    barrier = pltpu.get_barrier_semaphore()
    for step in range(1, count):
        pl.semaphore_signal(
            barrier, inc=1, device_id={axis: lax.rem(me + step, count)}, device_id_type=MESH
        )
    pl.semaphore_wait(barrier, count - 1)


def gather_kernel(count, own_ref, all_ref, send_sem, recv_sem):
    me = lax.axis_index("bl")
    greet("bl", me, count)
    copies = []
    for step in range(1, count):
        copy = pltpu.make_async_remote_copy(
            src_ref=own_ref,
            dst_ref=all_ref.at[me],
            send_sem=send_sem.at[step - 1],
            recv_sem=recv_sem.at[step - 1],
            device_id={"bl": lax.rem(me + step, count)},
            device_id_type=MESH,
        )
        copy.start()
        copies.append(copy)
    all_ref[me] = own_ref[...]
    for copy in copies:
        copy.wait()


def factor_table(first, rows, table, special):
    pixel = (first + lax.broadcasted_iota(jnp.int32, (rows, LANES), 0)).astype(jnp.float32)
    offset_lane = lax.broadcasted_iota(jnp.int32, (rows, LANES), 1)
    offset = (offset_lane % SUPPORT - SUPPORT // 2).astype(jnp.float32)
    cos_part, sin_part = turn_cos_sin(pixel * offset * (1.0 / GRID))
    if special:
        row = lax.broadcasted_iota(jnp.int32, (rows, LANES), 0)
        parity = 1.0 - 2.0 * (offset_lane % 2).astype(jnp.float32)
        sin_part = jnp.where(row == 0, parity, sin_part)
    table_high, table_low = split(table)

    def product(part):
        high, low = split(part)
        return dot_nt(high, table_high) + dot_nt(high, table_low) + dot_nt(low, table_high)

    return product(cos_part), product(sin_part)


def compute_kernel(
    layer_dev,
    pixels,
    blocks,
    depth_ref,
    table_ref,
    slots_ref,
    out_ref,
    table_pad,
    u_re,
    u_im,
    fine_re,
    fine_im,
    coarse_re,
    coarse_im,
    w_high,
    w_low,
    lhs_high,
    lhs_low,
    neg,
):
    half = GRID // 2
    tiles = slots_ref.shape[0]
    chunk_rows = GRID // blocks
    first_pixel = lax.axis_index("bl") * pixels
    table_pad[...] = jnp.zeros_like(table_pad)
    table_pad[0:OVERSAMPLE, 0:SUPPORT] = table_ref[...]
    table = table_pad[...]
    u_re[...], u_im[...] = factor_table(0, half, table, True)
    v_re, v_im = factor_table(first_pixel, pixels, table, False)
    fine_x = lax.broadcasted_iota(jnp.int32, (FINE, LANES), 0).astype(jnp.float32)
    coarse_x = (lax.broadcasted_iota(jnp.int32, (half // FINE, LANES), 0) * FINE).astype(
        jnp.float32
    )
    pixel_y = (
        first_pixel + lax.broadcasted_iota(jnp.int32, (pixels // FINE, LANES), 0) * FINE
    ).astype(jnp.float32)

    def prepare(tile, square):
        lanes = pl.ds(pl.multiple_of(tile * LANES, LANES), LANES)
        params = slots_ref[tile]
        vis_real, vis_imag, weight = params[0:1], params[1:2], params[2:3]
        row, col = params[3:4] * (1.0 / GRID), params[4:5] * (1.0 / GRID)
        col_kernel = params[6:7].astype(jnp.int32)
        layer = params[7:8]
        fine_re[:, lanes], fine_im[:, lanes] = turn_cos_sin(row * fine_x)
        coarse_re[:, lanes], coarse_im[:, lanes] = turn_cos_sin(row * coarse_x)
        cf_re, cf_im = turn_cos_sin(col * fine_x)
        cc_re, cc_im = turn_cos_sin(col * pixel_y)
        cv_re = cc_re * vis_real - cc_im * vis_imag
        cv_im = cc_re * vis_imag + cc_im * vis_real
        masks = [
            jnp.broadcast_to(jnp.where(layer == float(item), 1.0, 0.0), (FINE, LANES))
            for item in range(layer_dev)
        ]
        index = jnp.broadcast_to(col_kernel, (FINE, LANES))
        for group in range(pixels // FINE):
            rows = slice(group * FINE, (group + 1) * FINE)
            k_re = jnp.take_along_axis(v_re[rows], index, axis=1, mode="promise_in_bounds")
            k_im = jnp.take_along_axis(v_im[rows], index, axis=1, mode="promise_in_bounds")
            e_re = cf_re * cv_re[group : group + 1] - cf_im * cv_im[group : group + 1]
            e_im = cf_re * cv_im[group : group + 1] + cf_im * cv_re[group : group + 1]
            real = e_re * k_re - e_im * k_im
            imag = e_re * k_im + e_im * k_re
            for item in range(layer_dev):
                for place, value in enumerate((real, imag)):
                    high, low = split(value * masks[item])
                    start = (item * 2 + place) * pixels + group * FINE
                    w_high[start : start + FINE, lanes] = high
                    w_low[start : start + FINE, lanes] = low
        return square + weight * weight

    squares = lax.fori_loop(0, tiles, prepare, jnp.zeros((1, LANES), jnp.float32))
    square_sum = jnp.sum(squares)

    y_pixel = first_pixel + lax.broadcasted_iota(jnp.int32, (1, pixels), 1)
    y_coord = (y_pixel - GRID // 2).astype(jnp.float32) * (field_of_view / GRID)
    top_depth = jnp.sqrt(1.0 - y_coord * y_coord) - 1.0
    for block in range(half // XBLOCK):

        def expand(tile, carry):
            lanes = pl.ds(pl.multiple_of(tile * LANES, LANES), LANES)
            params = slots_ref[tile]
            index = jnp.broadcast_to(params[5:6].astype(jnp.int32), (FINE, LANES))
            f_re, f_im = fine_re[:, lanes], fine_im[:, lanes]
            c_re, c_im = coarse_re[:, lanes], coarse_im[:, lanes]
            for group in range(XBLOCK // FINE):
                place = block * (XBLOCK // FINE) + group
                rows = slice(place * FINE, (place + 1) * FINE)
                k_re = jnp.take_along_axis(u_re[rows, :], index, axis=1, mode="promise_in_bounds")
                k_im = jnp.take_along_axis(u_im[rows, :], index, axis=1, mode="promise_in_bounds")
                g_re, g_im = c_re[place : place + 1], c_im[place : place + 1]
                e_re = f_re * g_re - f_im * g_im
                e_im = f_re * g_im + f_im * g_re
                real = e_re * k_re - e_im * k_im
                imag = e_re * k_im + e_im * k_re
                if place == 0:
                    odd = params[3:4].astype(jnp.int32) % 2
                    sign = (1 - 2 * odd).astype(jnp.float32)
                    first_row = lax.broadcasted_iota(jnp.int32, (FINE, LANES), 0) == 0
                    imag = imag * jnp.where(first_row, sign, 1.0)
                for part, value in enumerate((real, imag)):
                    high, low = split(value)
                    start = part * XBLOCK + group * FINE
                    lhs_high[start : start + FINE, lanes] = high
                    lhs_low[start : start + FINE, lanes] = low
            return carry

        lax.fori_loop(0, tiles, expand, 0)
        product = (
            dot_nt(lhs_high[...], w_high[...])
            + dot_nt(lhs_high[...], w_low[...])
            + dot_nt(lhs_low[...], w_high[...])
        )
        x_row = block * XBLOCK + lax.broadcasted_iota(jnp.int32, (XBLOCK, 1), 0)
        x_coord = (x_row - GRID // 2).astype(jnp.float32) * (field_of_view / GRID)
        depth = jnp.sqrt(1.0 - x_coord * x_coord - y_coord * y_coord) - 1.0
        above = jnp.zeros((XBLOCK, pixels), jnp.float32)
        below = jnp.zeros((XBLOCK, pixels), jnp.float32)
        for item in range(layer_dev):
            first = item * 2 * pixels
            p_ac = product[:XBLOCK, first : first + pixels]
            p_ad = product[:XBLOCK, first + pixels : first + 2 * pixels]
            p_bc = product[XBLOCK:, first : first + pixels]
            p_bd = product[XBLOCK:, first + pixels : first + 2 * pixels]
            cos_part, sin_part = turn_cos_sin(depth_ref[item] * depth)
            if block == 0:
                top = x_row == 0
                top_cos, top_sin = turn_cos_sin(depth_ref[item] * top_depth)
                top_value = p_bc * top_cos - p_bd * top_sin
                p_bc = jnp.where(top, 0.0, p_bc)
                p_bd = jnp.where(top, 0.0, p_bd)
            above += (p_ac - p_bd) * cos_part - (p_ad + p_bc) * sin_part
            lower = (p_ac + p_bd) * cos_part - (p_ad - p_bc) * sin_part
            if block == 0:
                lower = jnp.where(top, top_value, lower)
            below += lower
        neg[block * XBLOCK : (block + 1) * XBLOCK, :] = below
        position = block * XBLOCK
        owner, inside = position // chunk_rows, position % chunk_rows
        for part in range(max(1, XBLOCK // chunk_rows)):
            size = min(XBLOCK, chunk_rows)
            out_ref[owner + part, inside : inside + size, :] = above[part * size : (part + 1) * size]
    parts = blocks // 2
    for part in range(parts):
        target = blocks - 1 - part
        out_ref[target, 0:chunk_rows, :] = neg[part * chunk_rows : (part + 1) * chunk_rows, :]
        source = (part + 1) % parts * chunk_rows
        out_ref[target, 0:1, :] = neg[source : source + 1, :]
    for target in range(blocks):
        out_ref[target, chunk_rows:, :] = jnp.full((8, pixels), square_sum, jnp.float32)


def reduce_kernel(count, own_ref, out_ref, held, send_sem, recv_sem):
    me = lax.axis_index("wa")
    rows = out_ref.shape[0]
    greet("wa", me, count)
    copies = []
    for step in range(1, count):
        peer = lax.rem(me + step, count)
        copy = pltpu.make_async_remote_copy(
            src_ref=own_ref.at[peer],
            dst_ref=held.at[step - 1],
            send_sem=send_sem.at[step - 1],
            recv_sem=recv_sem.at[step - 1],
            device_id={"wa": peer},
            device_id_type=MESH,
        )
        copy.start()
        copies.append(copy)
    total = own_ref[me]
    for step, copy in enumerate(copies):
        copy.wait()
        total = total + held[step]
    value = total[:rows] / jnp.sqrt(total[rows : rows + 1])
    out_row = lax.broadcasted_iota(jnp.int32, (rows, rows), 0)
    in_row = lax.broadcasted_iota(jnp.int32, (rows, rows), 1)
    turned = jnp.where(me * 2 >= count, (rows - out_row) % rows, out_row)
    chosen = jnp.where(turned == in_row, 1.0, 0.0).astype(jnp.bfloat16)
    high, rest = split(value)
    low, last = split(value - high.astype(jnp.float32))
    out_ref[...] = sum(
        jnp.dot(chosen, piece, preferred_element_type=jnp.float32) for piece in (high, low, last)
    )


def body(
    visibilities,
    weights,
    cell_index,
    kernel_index,
    layer_index,
    tile_counts,
    kernel_table,
    layer_depth,
):
    layer_dev = layer_depth.shape[0]
    peers = lax.axis_size("bl")
    blocks = lax.axis_size("wa")
    pixels = GRID // peers
    chunk_rows = GRID // blocks
    tiles = cell_index.shape[1]
    position = lax.broadcasted_iota(jnp.int32, cell_index.shape, 2)
    used_weight = jnp.where(position < tile_counts[:, :, None], weights, 0.0)
    packed = jnp.stack(
        [
            visibilities[0, :, 0, :] * used_weight[0],
            visibilities[0, :, 1, :] * used_weight[0],
            used_weight[0],
            (cell_index[0] // GRID).astype(jnp.float32),
            (cell_index[0] % GRID).astype(jnp.float32),
            (kernel_index[0] // OVERSAMPLE).astype(jnp.float32),
            (kernel_index[0] % OVERSAMPLE).astype(jnp.float32),
            layer_index[0].astype(jnp.float32),
        ],
        axis=1,
    )
    vmem = pl.BlockSpec(memory_space=pltpu.VMEM)
    smem = pl.BlockSpec(memory_space=pltpu.SMEM)
    slots = pl.pallas_call(
        functools.partial(gather_kernel, peers),
        out_shape=jax.ShapeDtypeStruct((peers, tiles, 8, LANES), jnp.float32),
        in_specs=[vmem],
        out_specs=vmem,
        scratch_shapes=[
            pltpu.SemaphoreType.DMA((peers - 1,)),
            pltpu.SemaphoreType.DMA((peers - 1,)),
        ],
        compiler_params=pltpu.CompilerParams(collective_id=0, has_side_effects=True),
        name="gather_slots",
    )(packed)
    slots = slots.reshape(peers * tiles, 8, LANES)
    count = peers * tiles * LANES
    half = GRID // 2
    columns = 2 * layer_dev * pixels
    partial_image = pl.pallas_call(
        functools.partial(compute_kernel, layer_dev, pixels, blocks),
        out_shape=jax.ShapeDtypeStruct((blocks, chunk_rows + 8, pixels), jnp.float32),
        in_specs=[smem, vmem, vmem],
        out_specs=vmem,
        scratch_shapes=[
            pltpu.VMEM((LANES, LANES), jnp.float32),
            pltpu.VMEM((half, LANES), jnp.float32),
            pltpu.VMEM((half, LANES), jnp.float32),
            pltpu.VMEM((FINE, count), jnp.float32),
            pltpu.VMEM((FINE, count), jnp.float32),
            pltpu.VMEM((half // FINE, count), jnp.float32),
            pltpu.VMEM((half // FINE, count), jnp.float32),
            pltpu.VMEM((columns, count), jnp.bfloat16),
            pltpu.VMEM((columns, count), jnp.bfloat16),
            pltpu.VMEM((2 * XBLOCK, count), jnp.bfloat16),
            pltpu.VMEM((2 * XBLOCK, count), jnp.bfloat16),
            pltpu.VMEM((half, pixels), jnp.float32),
        ],
        compiler_params=pltpu.CompilerParams(vmem_limit_bytes=48 * 1024 * 1024),
        name="image_block",
    )(layer_depth, kernel_table, slots)
    return pl.pallas_call(
        functools.partial(reduce_kernel, blocks),
        out_shape=jax.ShapeDtypeStruct((chunk_rows, pixels), jnp.float32),
        in_specs=[vmem],
        out_specs=vmem,
        scratch_shapes=[
            pltpu.VMEM((blocks - 1, chunk_rows + 8, pixels), jnp.float32),
            pltpu.SemaphoreType.DMA((blocks - 1,)),
            pltpu.SemaphoreType.DMA((blocks - 1,)),
        ],
        compiler_params=pltpu.CompilerParams(collective_id=1, has_side_effects=True),
        name="sum_layers",
    )(partial_image)


def solution(mesh):
    in_specs = (
        P("wa", "bl", None, None),
        P("wa", "bl", None),
        P("wa", "bl", None),
        P("wa", "bl", None),
        P("wa", "bl", None),
        P("wa", "bl"),
        P(),
        P("wa"),
    )
    out_specs = P("wa", "bl")
    return jax.shard_map(body, mesh=mesh, in_specs=in_specs, out_specs=out_specs, check_vma=False)
```

```python
import functools
import math

import jax
import jax.numpy as jnp
from jax import lax
from jax.experimental import pallas as pl
from jax.experimental.pallas import tpu as pltpu
from jax.sharding import PartitionSpec as P

GRID = 1024
SUPPORT = 8
OVERSAMPLE = 16
LANES = 128
FINE = 32
XBLOCK = 128
CHUNK = 2 * LANES
PIECES = 3

field_of_view = 0.6
MESH = pl.DeviceIdType.MESH

TWO_PI = 2.0 * math.pi
SIN_TERMS = [(-1) ** k * TWO_PI ** (2 * k + 1) / math.factorial(2 * k + 1) for k in range(9)]
COS_TERMS = [(-1) ** k * TWO_PI ** (2 * k) / math.factorial(2 * k) for k in range(10)]


def horner(square, terms):
    value = jnp.full_like(square, terms[-1])
    for term in terms[-2::-1]:
        value = value * square + term
    return value


def turn_cos_sin(turns):
    part = turns - jnp.round(turns)
    square = part * part
    return horner(square, COS_TERMS), part * horner(square, SIN_TERMS)


def split(value):
    high = value.astype(jnp.bfloat16)
    return high, (value - high.astype(jnp.float32)).astype(jnp.bfloat16)


def dot_nt(a, b):
    return lax.dot_general(
        a, b, (((1,), (1,)), ((), ())), preferred_element_type=jnp.float32
    )


def factor_table(first, rows, table, special):
    pixel = (first + lax.broadcasted_iota(jnp.int32, (rows, LANES), 0)).astype(jnp.float32)
    offset_lane = lax.broadcasted_iota(jnp.int32, (rows, LANES), 1)
    offset = (offset_lane % SUPPORT - SUPPORT // 2).astype(jnp.float32)
    cos_part, sin_part = turn_cos_sin(pixel * offset * (1.0 / GRID))
    if special:
        row = lax.broadcasted_iota(jnp.int32, (rows, LANES), 0)
        parity = 1.0 - 2.0 * (offset_lane % 2).astype(jnp.float32)
        sin_part = jnp.where(row == 0, parity, sin_part)
    table_high, table_low = split(table)

    def product(part):
        high, low = split(part)
        return dot_nt(high, table_high) + dot_nt(high, table_low) + dot_nt(low, table_high)

    return product(cos_part), product(sin_part)


def start_all(copies):
    for copy in copies:
        copy.start()


def kernel(
    layer_dev,
    pixels,
    blocks,
    peers,
    depth_ref,
    counts_ref,
    table_ref,
    vis_ref,
    weight_ref,
    cell_ref,
    index_ref,
    layer_ref,
    out_ref,
    own,
    slots_ref,
    table_pad,
    u_re,
    u_im,
    v_re,
    v_im,
    fine_re,
    fine_im,
    coarse_re,
    coarse_im,
    rhs,
    lhs,
    acc,
    image,
    tail,
    held,
    held_tail,
    slot_send,
    slot_recv,
    image_send,
    image_recv,
    tail_send,
    tail_recv,
):
    half = GRID // 2
    chunk_rows = GRID // blocks
    own_tiles = own.shape[0]
    tiles = peers * own_tiles
    block_total = half // XBLOCK
    subs = chunk_rows // XBLOCK
    me_bl, me_wa = lax.axis_index("bl"), lax.axis_index("wa")
    barrier = pltpu.get_barrier_semaphore()
    for axis, me, count in (("bl", me_bl, peers), ("wa", me_wa, blocks)):
        for step in range(1, count):
            pl.semaphore_signal(
                barrier, inc=1, device_id={axis: lax.rem(me + step, count)}, device_id_type=MESH
            )
    position = lax.broadcasted_iota(jnp.int32, (1, LANES), 1)
    for tile in range(own_tiles):
        line = slice(tile, tile + 1)
        weight = jnp.where(position < counts_ref[0, tile], weight_ref[0, line], 0.0)
        cell, index = cell_ref[0, line], index_ref[0, line]
        values = [
            vis_ref[0, tile, 0:1] * weight,
            vis_ref[0, tile, 1:2] * weight,
            weight,
            (cell // GRID).astype(jnp.float32),
            (cell % GRID).astype(jnp.float32),
            (index // OVERSAMPLE).astype(jnp.float32),
            (index % OVERSAMPLE).astype(jnp.float32),
            layer_ref[0, line].astype(jnp.float32),
        ]
        for place, value in enumerate(values):
            own[tile, place : place + 1] = value
    pl.semaphore_wait(barrier, peers + blocks - 2)
    slot_copies = [
        pltpu.make_async_remote_copy(
            src_ref=own,
            dst_ref=slots_ref.at[pl.ds(me_bl * own_tiles, own_tiles)],
            send_sem=slot_send.at[step - 1],
            recv_sem=slot_recv.at[step - 1],
            device_id={"bl": lax.rem(me_bl + step, peers)},
            device_id_type=MESH,
        )
        for step in range(1, peers)
    ]
    start_all(slot_copies)
    slots_ref[pl.ds(me_bl * own_tiles, own_tiles)] = own[...]

    first_pixel = me_bl * pixels
    table_pad[...] = jnp.zeros_like(table_pad)
    table_pad[0:OVERSAMPLE, 0:SUPPORT] = table_ref[...]
    table = table_pad[...]
    u_re[...], u_im[...] = factor_table(0, half, table, True)
    v_re[...], v_im[...] = factor_table(first_pixel, pixels, table, False)
    fine_x = lax.broadcasted_iota(jnp.int32, (FINE, LANES), 0).astype(jnp.float32)
    coarse_x = (lax.broadcasted_iota(jnp.int32, (half // FINE, LANES), 0) * FINE).astype(
        jnp.float32
    )
    pixel_y = (
        first_pixel + lax.broadcasted_iota(jnp.int32, (pixels // FINE, LANES), 0) * FINE
    ).astype(jnp.float32)
    for copy in slot_copies:
        copy.wait()

    def lanes_of(tile):
        return pl.ds(pl.multiple_of(tile * LANES, LANES), LANES)

    def piece_lanes(tile):
        base = tile // 2 * (PIECES * CHUNK) + tile % 2 * LANES
        return [
            pl.ds(pl.multiple_of(base + piece * CHUNK, LANES), LANES) for piece in range(PIECES)
        ]

    def prepare(tile, square):
        lanes = lanes_of(tile)
        places = piece_lanes(tile)
        params = slots_ref[tile]
        vis_real, vis_imag, weight = params[0:1], params[1:2], params[2:3]
        row, col = params[3:4] * (1.0 / GRID), params[4:5] * (1.0 / GRID)
        col_kernel = params[6:7].astype(jnp.int32)
        layer = params[7:8]
        fine_re[:, lanes], fine_im[:, lanes] = turn_cos_sin(row * fine_x)
        coarse_re[:, lanes], coarse_im[:, lanes] = turn_cos_sin(row * coarse_x)
        cf_re, cf_im = turn_cos_sin(col * fine_x)
        cc_re, cc_im = turn_cos_sin(col * pixel_y)
        cv_re = cc_re * vis_real - cc_im * vis_imag
        cv_im = cc_re * vis_imag + cc_im * vis_real
        masks = [
            jnp.broadcast_to(jnp.where(layer == float(item), 1.0, 0.0), (FINE, LANES))
            for item in range(layer_dev)
        ]
        index = jnp.broadcast_to(col_kernel, (FINE, LANES))
        for group in range(pixels // FINE):
            rows = slice(group * FINE, (group + 1) * FINE)
            k_re = jnp.take_along_axis(v_re[rows, :], index, axis=1, mode="promise_in_bounds")
            k_im = jnp.take_along_axis(v_im[rows, :], index, axis=1, mode="promise_in_bounds")
            e_re = cf_re * cv_re[group : group + 1] - cf_im * cv_im[group : group + 1]
            e_im = cf_re * cv_im[group : group + 1] + cf_im * cv_re[group : group + 1]
            real = e_re * k_re - e_im * k_im
            imag = e_re * k_im + e_im * k_re
            for item in range(layer_dev):
                for place, value in enumerate((real, imag)):
                    high, low = split(value * masks[item])
                    start = (item * 2 + place) * pixels + group * FINE
                    for where, piece in zip(places, (high, low, high)):
                        rhs[start : start + FINE, where] = piece
        return square + weight * weight

    squares = lax.fori_loop(0, tiles, prepare, jnp.zeros((1, LANES), jnp.float32))
    square_sum = jnp.sum(squares)

    def expand(block, tile):
        lanes = lanes_of(tile)
        places = piece_lanes(tile)
        params = slots_ref[tile]
        index = jnp.broadcast_to(params[5:6].astype(jnp.int32), (FINE, LANES))
        f_re, f_im = fine_re[:, lanes], fine_im[:, lanes]
        for group in range(XBLOCK // FINE):
            place = block * (XBLOCK // FINE) + group
            rows = slice(place * FINE, (place + 1) * FINE)
            k_re = jnp.take_along_axis(u_re[rows, :], index, axis=1, mode="promise_in_bounds")
            k_im = jnp.take_along_axis(u_im[rows, :], index, axis=1, mode="promise_in_bounds")
            g_re = coarse_re[place : place + 1, lanes]
            g_im = coarse_im[place : place + 1, lanes]
            e_re = f_re * g_re - f_im * g_im
            e_im = f_re * g_im + f_im * g_re
            real = e_re * k_re - e_im * k_im
            imag = e_re * k_im + e_im * k_re
            if place == 0:
                odd = params[3:4].astype(jnp.int32) % 2
                sign = (1 - 2 * odd).astype(jnp.float32)
                first_row = lax.broadcasted_iota(jnp.int32, (FINE, LANES), 0) == 0
                imag = imag * jnp.where(first_row, sign, 1.0)
            for part, value in enumerate((real, imag)):
                high, low = split(value)
                start = part * XBLOCK + group * FINE
                for where, piece in zip(places, (high, high, low)):
                    lhs[block % 2, start : start + FINE, where] = piece

    def image_copy(owner, sub):
        slot = lax.rem(owner - me_wa + blocks, blocks) - 1
        rows = pl.ds(sub * XBLOCK, XBLOCK)
        return pltpu.make_async_remote_copy(
            src_ref=image.at[owner, rows],
            dst_ref=held.at[slot, rows],
            send_sem=image_send.at[owner, sub],
            recv_sem=image_recv.at[slot, sub],
            device_id={"wa": owner},
            device_id_type=MESH,
        )

    def tail_copy(step):
        peer = lax.rem(me_wa + step, blocks)
        return pltpu.make_async_remote_copy(
            src_ref=tail.at[peer],
            dst_ref=held_tail.at[step - 1],
            send_sem=tail_send.at[step - 1],
            recv_sem=tail_recv.at[step - 1],
            device_id={"wa": peer},
            device_id_type=MESH,
        )

    y_pixel = first_pixel + lax.broadcasted_iota(jnp.int32, (1, pixels), 1)
    y_coord = (y_pixel - GRID // 2).astype(jnp.float32) * (field_of_view / GRID)
    top_depth = jnp.sqrt(1.0 - y_coord * y_coord) - 1.0
    tail[...] = jnp.full_like(tail, square_sum)

    @pl.loop(0, tiles)
    def _(tile):
        expand(0, tile)

    parts = blocks // 2
    for block in range(block_total):

        @pl.loop(0, tiles // 2)
        def _(chunk):
            wide = pl.ds(pl.multiple_of(chunk * (PIECES * CHUNK), LANES), PIECES * CHUNK)
            product = dot_nt(lhs[block % 2, :, wide], rhs[:, wide])
            if block + 1 < block_total:
                expand(block + 1, chunk * 2)
                expand(block + 1, chunk * 2 + 1)
            acc[...] = jnp.where(chunk == 0, 0.0, acc[...]) + product

        x_row = block * XBLOCK + lax.broadcasted_iota(jnp.int32, (XBLOCK, 1), 0)
        x_coord = (x_row - GRID // 2).astype(jnp.float32) * (field_of_view / GRID)
        depth = jnp.sqrt(1.0 - x_coord * x_coord - y_coord * y_coord) - 1.0
        above = jnp.zeros((XBLOCK, pixels), jnp.float32)
        below = jnp.zeros((XBLOCK, pixels), jnp.float32)
        for item in range(layer_dev):
            first = item * 2 * pixels
            p_ac = acc[:XBLOCK, first : first + pixels]
            p_ad = acc[:XBLOCK, first + pixels : first + 2 * pixels]
            p_bc = acc[XBLOCK:, first : first + pixels]
            p_bd = acc[XBLOCK:, first + pixels : first + 2 * pixels]
            cos_part, sin_part = turn_cos_sin(depth_ref[item] * depth)
            if block == 0:
                top = x_row == 0
                top_cos, top_sin = turn_cos_sin(depth_ref[item] * top_depth)
                top_value = p_bc * top_cos - p_bd * top_sin
                p_bc = jnp.where(top, 0.0, p_bc)
                p_bd = jnp.where(top, 0.0, p_bd)
            above += (p_ac - p_bd) * cos_part - (p_ad + p_bc) * sin_part
            lower = (p_ac + p_bd) * cos_part - (p_ad - p_bc) * sin_part
            if block == 0:
                lower = jnp.where(top, top_value, lower)
            below += lower
        part, sub = block // subs, block % subs
        rows = slice(sub * XBLOCK, (sub + 1) * XBLOCK)
        for owner, value in ((part, above), (blocks - 1 - part, below)):
            image[owner, rows, :] = value

            @pl.when(me_wa != owner)
            def _():
                image_copy(owner, sub).start()

        if sub == 0:
            target = blocks - 1 - (part - 1) % parts
            tail[target, 1:2, :] = below[0:1]

    tail_copies = [tail_copy(step) for step in range(1, blocks)]
    start_all(tail_copies)
    total = image[me_wa]
    total_tail = tail[me_wa]
    for step in range(1, blocks):
        for sub in range(subs):
            rows = pl.ds(sub * XBLOCK, XBLOCK)
            pltpu.make_async_remote_copy(
                src_ref=image.at[me_wa, rows],
                dst_ref=held.at[step - 1, rows],
                send_sem=image_send.at[me_wa, sub],
                recv_sem=image_recv.at[step - 1, sub],
                device_id={"wa": lax.rem(me_wa + step, blocks)},
                device_id_type=MESH,
            ).wait_recv()
        total = total + held[step - 1]
    for step, copy in enumerate(tail_copies):
        copy.wait()
        total_tail = total_tail + held_tail[step]
    scale = 1.0 / jnp.sqrt(total_tail[0:1])
    out_row = lax.broadcasted_iota(jnp.int32, (chunk_rows, chunk_rows), 0)
    in_row = lax.broadcasted_iota(jnp.int32, (chunk_rows, chunk_rows), 1)
    mirrored = me_wa * 2 >= blocks
    turned = jnp.where(mirrored, (chunk_rows - out_row) % chunk_rows, out_row)
    chosen = jnp.where(turned == in_row, 1.0, 0.0).astype(jnp.bfloat16)
    high, rest = split(total)
    low, last = split(total - high.astype(jnp.float32))
    ordered = sum(
        jnp.dot(chosen, piece, preferred_element_type=jnp.float32) for piece in (high, low, last)
    )
    out_line = lax.broadcasted_iota(jnp.int32, (chunk_rows, 1), 0)
    swap = jnp.where(mirrored, out_line, 1) == 0
    out_ref[...] = jnp.where(swap, total_tail[1:2], ordered) * scale
    for owner in range(blocks):

        @pl.when(me_wa != owner)
        def _():
            for sub in range(subs):
                image_copy(owner, sub).wait_send()


def body(
    visibilities,
    weights,
    cell_index,
    kernel_index,
    layer_index,
    tile_counts,
    kernel_table,
    layer_depth,
):
    layer_dev = layer_depth.shape[0]
    peers = lax.axis_size("bl")
    blocks = lax.axis_size("wa")
    pixels = GRID // peers
    chunk_rows = GRID // blocks
    own_tiles = cell_index.shape[1]
    tiles = peers * own_tiles
    count = tiles * LANES
    half = GRID // 2
    columns = 2 * layer_dev * pixels
    vmem = pl.BlockSpec(memory_space=pltpu.VMEM)
    smem = pl.BlockSpec(memory_space=pltpu.SMEM)
    f32, bf16 = jnp.float32, jnp.bfloat16
    shapes = [
        ((own_tiles, 8, LANES), f32),
        ((tiles, 8, LANES), f32),
        ((LANES, LANES), f32),
        ((half, LANES), f32),
        ((half, LANES), f32),
        ((pixels, LANES), f32),
        ((pixels, LANES), f32),
        ((FINE, count), f32),
        ((FINE, count), f32),
        ((half // FINE, count), f32),
        ((half // FINE, count), f32),
        ((columns, PIECES * count), bf16),
        ((2, 2 * XBLOCK, PIECES * count), bf16),
        ((2 * XBLOCK, columns), f32),
        ((blocks, chunk_rows, pixels), f32),
        ((blocks, 8, pixels), f32),
        ((blocks - 1, chunk_rows, pixels), f32),
        ((blocks - 1, 8, pixels), f32),
    ]
    subs = chunk_rows // XBLOCK
    semaphores = [
        (peers - 1,),
        (peers - 1,),
        (blocks, subs),
        (blocks - 1, subs),
        (blocks - 1,),
        (blocks - 1,),
    ]
    return pl.pallas_call(
        functools.partial(kernel, layer_dev, pixels, blocks, peers),
        out_shape=jax.ShapeDtypeStruct((chunk_rows, pixels), f32),
        in_specs=[smem, smem] + [vmem] * 6,
        out_specs=vmem,
        scratch_shapes=[pltpu.VMEM(shape, kind) for shape, kind in shapes]
        + [pltpu.SemaphoreType.DMA(shape) for shape in semaphores],
        compiler_params=pltpu.CompilerParams(
            collective_id=0, has_side_effects=True, vmem_limit_bytes=48 * 1024 * 1024
        ),
        name="dirty_image",
    )(
        layer_depth,
        tile_counts,
        kernel_table,
        visibilities,
        weights,
        cell_index,
        kernel_index,
        layer_index,
    )


def solution(mesh):
    in_specs = (
        P("wa", "bl", None, None),
        P("wa", "bl", None),
        P("wa", "bl", None),
        P("wa", "bl", None),
        P("wa", "bl", None),
        P("wa", "bl"),
        P(),
        P("wa"),
    )
    out_specs = P("wa", "bl")
    return jax.shard_map(body, mesh=mesh, in_specs=in_specs, out_specs=out_specs, check_vma=False)
```

```python
import functools
import math

import jax
import jax.numpy as jnp
from jax import lax
from jax.experimental import pallas as pl
from jax.experimental.pallas import tpu as pltpu
from jax.sharding import PartitionSpec as P

GRID = 1024
SUPPORT = 8
OVERSAMPLE = 16
LANES = 128
FINE = 32
XBLOCK = 128
CHUNK = 2 * LANES
PIECES = 3

field_of_view = 0.6
MESH = pl.DeviceIdType.MESH

TWO_PI = 2.0 * math.pi
SIN_TERMS = [(-1) ** k * TWO_PI ** (2 * k + 1) / math.factorial(2 * k + 1) for k in range(9)]
COS_TERMS = [(-1) ** k * TWO_PI ** (2 * k) / math.factorial(2 * k) for k in range(10)]


def horner(square, terms):
    value = jnp.full_like(square, terms[-1])
    for term in terms[-2::-1]:
        value = value * square + term
    return value


def turn_cos_sin(turns):
    part = turns - jnp.round(turns)
    square = part * part
    return horner(square, COS_TERMS), part * horner(square, SIN_TERMS)


def split(value):
    high = value.astype(jnp.bfloat16)
    return high, (value - high.astype(jnp.float32)).astype(jnp.bfloat16)


def dot_nt(a, b):
    return lax.dot_general(
        a, b, (((1,), (1,)), ((), ())), preferred_element_type=jnp.float32
    )


def factor_table(first, rows, table, special):
    pixel = (first + lax.broadcasted_iota(jnp.int32, (rows, LANES), 0)).astype(jnp.float32)
    offset_lane = lax.broadcasted_iota(jnp.int32, (rows, LANES), 1)
    offset = (offset_lane % SUPPORT - SUPPORT // 2).astype(jnp.float32)
    cos_part, sin_part = turn_cos_sin(pixel * offset * (1.0 / GRID))
    if special:
        row = lax.broadcasted_iota(jnp.int32, (rows, LANES), 0)
        parity = 1.0 - 2.0 * (offset_lane % 2).astype(jnp.float32)
        sin_part = jnp.where(row == 0, parity, sin_part)
    table_high, table_low = split(table)

    def product(part):
        high, low = split(part)
        return dot_nn(high, table_high) + dot_nn(high, table_low) + dot_nn(low, table_high)

    return product(cos_part), product(sin_part)


def dot_nn(a, b):
    return jnp.dot(a, b, preferred_element_type=jnp.float32)


def start_all(copies):
    for copy in copies:
        copy.start()


def kernel(
    layer_dev,
    pixels,
    blocks,
    peers,
    depth_hbm,
    counts_hbm,
    table_hbm,
    vis_hbm,
    weight_hbm,
    cell_hbm,
    index_hbm,
    layer_hbm,
    out_ref,
    depth_ref,
    counts_ref,
    table_ref,
    vis_ref,
    weight_ref,
    cell_ref,
    index_ref,
    layer_ref,
    load_sem,
    own,
    slots_ref,
    table_pad,
    u_re,
    u_im,
    v_re,
    v_im,
    fine_re,
    fine_im,
    coarse_re,
    coarse_im,
    rhs,
    lhs,
    acc,
    image,
    tail,
    held,
    held_tail,
    slot_send,
    slot_recv,
    image_send,
    image_recv,
    tail_send,
    tail_recv,
):
    half = GRID // 2
    chunk_rows = GRID // blocks
    own_tiles = own.shape[0]
    tiles = peers * own_tiles
    block_total = half // XBLOCK
    subs = chunk_rows // XBLOCK
    me_bl, me_wa = lax.axis_index("bl"), lax.axis_index("wa")
    loads = [
        pltpu.make_async_copy(source, target, load_sem.at[place])
        for place, (source, target) in enumerate(
            (
                (counts_hbm, counts_ref),
                (vis_hbm, vis_ref),
                (weight_hbm, weight_ref),
                (cell_hbm, cell_ref),
                (index_hbm, index_ref),
                (layer_hbm, layer_ref),
                (table_hbm, table_ref),
                (depth_hbm, depth_ref),
            )
        )
    ]
    start_all(loads)
    barrier = pltpu.get_barrier_semaphore()
    for axis, me, count in (("bl", me_bl, peers), ("wa", me_wa, blocks)):
        for step in range(1, count):
            pl.semaphore_signal(
                barrier, inc=1, device_id={axis: lax.rem(me + step, count)}, device_id_type=MESH
            )
    for load in loads:
        load.wait()
    position = lax.broadcasted_iota(jnp.int32, (1, LANES), 1)
    for tile in range(own_tiles):
        line = slice(tile, tile + 1)
        weight = jnp.where(position < counts_ref[0:1, tile : tile + 1], weight_ref[0, line], 0.0)
        cell, index = cell_ref[0, line], index_ref[0, line]
        values = [
            vis_ref[0, tile, 0:1] * weight,
            vis_ref[0, tile, 1:2] * weight,
            weight,
            (cell // GRID).astype(jnp.float32),
            (cell % GRID).astype(jnp.float32),
            (index // OVERSAMPLE).astype(jnp.float32),
            (index % OVERSAMPLE).astype(jnp.float32),
            layer_ref[0, line].astype(jnp.float32),
        ]
        for place, value in enumerate(values):
            own[tile, place : place + 1] = value
    pl.semaphore_wait(barrier, peers + blocks - 2)
    slot_copies = [
        pltpu.make_async_remote_copy(
            src_ref=own,
            dst_ref=slots_ref.at[pl.ds(me_bl * own_tiles, own_tiles)],
            send_sem=slot_send.at[step - 1],
            recv_sem=slot_recv.at[step - 1],
            device_id={"bl": lax.rem(me_bl + step, peers)},
            device_id_type=MESH,
        )
        for step in range(1, peers)
    ]
    start_all(slot_copies)
    slots_ref[pl.ds(me_bl * own_tiles, own_tiles)] = own[...]

    first_pixel = me_bl * pixels
    table_pad[...] = jnp.zeros_like(table_pad)
    table_pad[0:SUPPORT, 0:OVERSAMPLE] = table_ref[...]
    table = table_pad[...]
    u_re[...], u_im[...] = factor_table(0, half, table, True)
    v_re[...], v_im[...] = factor_table(first_pixel, pixels, table, False)
    fine_x = lax.broadcasted_iota(jnp.int32, (FINE, LANES), 0).astype(jnp.float32)
    coarse_x = (lax.broadcasted_iota(jnp.int32, (half // FINE, LANES), 0) * FINE).astype(
        jnp.float32
    )
    pixel_y = (
        first_pixel + lax.broadcasted_iota(jnp.int32, (pixels // FINE, LANES), 0) * FINE
    ).astype(jnp.float32)
    for copy in slot_copies:
        copy.wait()

    def lanes_of(tile):
        return pl.ds(pl.multiple_of(tile * LANES, LANES), LANES)

    def piece_lanes(tile):
        base = tile // 2 * (PIECES * CHUNK) + tile % 2 * LANES
        return [
            pl.ds(pl.multiple_of(base + piece * CHUNK, LANES), LANES) for piece in range(PIECES)
        ]

    def prepare(tile, square):
        lanes = lanes_of(tile)
        places = piece_lanes(tile)
        params = slots_ref[tile]
        vis_real, vis_imag, weight = params[0:1], params[1:2], params[2:3]
        row, col = params[3:4] * (1.0 / GRID), params[4:5] * (1.0 / GRID)
        col_kernel = params[6:7].astype(jnp.int32)
        layer = params[7:8]
        fine_re[:, lanes], fine_im[:, lanes] = turn_cos_sin(row * fine_x)
        coarse_re[:, lanes], coarse_im[:, lanes] = turn_cos_sin(row * coarse_x)
        cf_re, cf_im = turn_cos_sin(col * fine_x)
        cc_re, cc_im = turn_cos_sin(col * pixel_y)
        cv_re = cc_re * vis_real - cc_im * vis_imag
        cv_im = cc_re * vis_imag + cc_im * vis_real
        masks = [
            jnp.broadcast_to(jnp.where(layer == float(item), 1.0, 0.0), (FINE, LANES))
            for item in range(layer_dev)
        ]
        index = jnp.broadcast_to(col_kernel, (FINE, LANES))
        for group in range(pixels // FINE):
            rows = slice(group * FINE, (group + 1) * FINE)
            k_re = jnp.take_along_axis(v_re[rows, :], index, axis=1, mode="promise_in_bounds")
            k_im = jnp.take_along_axis(v_im[rows, :], index, axis=1, mode="promise_in_bounds")
            e_re = cf_re * cv_re[group : group + 1] - cf_im * cv_im[group : group + 1]
            e_im = cf_re * cv_im[group : group + 1] + cf_im * cv_re[group : group + 1]
            real = e_re * k_re - e_im * k_im
            imag = e_re * k_im + e_im * k_re
            for item in range(layer_dev):
                for place, value in enumerate((real, imag)):
                    high, low = split(value * masks[item])
                    start = (item * 2 + place) * pixels + group * FINE
                    for where, piece in zip(places, (high, low, high)):
                        rhs[start : start + FINE, where] = piece
        return square + weight * weight

    squares = lax.fori_loop(0, tiles, prepare, jnp.zeros((1, LANES), jnp.float32))
    square_sum = jnp.sum(squares)

    def expand(block, side, tile):
        lanes = lanes_of(tile)
        places = piece_lanes(tile)
        params = slots_ref[tile]
        index = jnp.broadcast_to(params[5:6].astype(jnp.int32), (FINE, LANES))
        f_re, f_im = fine_re[:, lanes], fine_im[:, lanes]
        for group in range(XBLOCK // FINE):
            place = block * (XBLOCK // FINE) + group
            rows = slice(place * FINE, (place + 1) * FINE)
            k_re = jnp.take_along_axis(u_re[rows, :], index, axis=1, mode="promise_in_bounds")
            k_im = jnp.take_along_axis(u_im[rows, :], index, axis=1, mode="promise_in_bounds")
            g_re = coarse_re[place : place + 1, lanes]
            g_im = coarse_im[place : place + 1, lanes]
            e_re = f_re * g_re - f_im * g_im
            e_im = f_re * g_im + f_im * g_re
            real = e_re * k_re - e_im * k_im
            imag = e_re * k_im + e_im * k_re
            if place == 0:
                odd = params[3:4].astype(jnp.int32) % 2
                sign = (1 - 2 * odd).astype(jnp.float32)
                first_row = lax.broadcasted_iota(jnp.int32, (FINE, LANES), 0) == 0
                imag = imag * jnp.where(first_row, sign, 1.0)
            for part, value in enumerate((real, imag)):
                high, low = split(value)
                start = part * XBLOCK + group * FINE
                for where, piece in zip(places, (high, high, low)):
                    lhs[side, start : start + FINE, where] = piece

    def image_copy(owner, sub):
        slot = lax.rem(owner - me_wa + blocks, blocks) - 1
        rows = pl.ds(sub * XBLOCK, XBLOCK)
        return pltpu.make_async_remote_copy(
            src_ref=image.at[owner, rows],
            dst_ref=held.at[slot, rows],
            send_sem=image_send.at[owner, sub],
            recv_sem=image_recv.at[slot, sub],
            device_id={"wa": owner},
            device_id_type=MESH,
        )

    def tail_copy(step):
        peer = lax.rem(me_wa + step, blocks)
        return pltpu.make_async_remote_copy(
            src_ref=tail.at[peer],
            dst_ref=held_tail.at[step - 1],
            send_sem=tail_send.at[step - 1],
            recv_sem=tail_recv.at[step - 1],
            device_id={"wa": peer},
            device_id_type=MESH,
        )

    y_pixel = first_pixel + lax.broadcasted_iota(jnp.int32, (1, pixels), 1)
    y_coord = (y_pixel - GRID // 2).astype(jnp.float32) * (field_of_view / GRID)
    top_depth = jnp.sqrt(1.0 - y_coord * y_coord) - 1.0
    tail[...] = jnp.full_like(tail, square_sum)

    @pl.loop(0, tiles)
    def _(tile):
        expand(0, 0, tile)

    parts = blocks // 2
    order = [first + part * subs for first in range(subs) for part in range(block_total // subs)]
    for turn, block in enumerate(order):
        following = order[turn + 1] if turn + 1 < block_total else None

        @pl.loop(0, tiles // 2)
        def _(chunk):
            wide = pl.ds(pl.multiple_of(chunk * (PIECES * CHUNK), LANES), PIECES * CHUNK)
            product = dot_nt(lhs[turn % 2, :, wide], rhs[:, wide])
            if following is not None:
                expand(following, (turn + 1) % 2, chunk * 2)
                expand(following, (turn + 1) % 2, chunk * 2 + 1)
            acc[...] = jnp.where(chunk == 0, 0.0, acc[...]) + product

        x_row = block * XBLOCK + lax.broadcasted_iota(jnp.int32, (XBLOCK, 1), 0)
        x_coord = (x_row - GRID // 2).astype(jnp.float32) * (field_of_view / GRID)
        depth = jnp.sqrt(1.0 - x_coord * x_coord - y_coord * y_coord) - 1.0
        above = jnp.zeros((XBLOCK, pixels), jnp.float32)
        below = jnp.zeros((XBLOCK, pixels), jnp.float32)
        for item in range(layer_dev):
            first = item * 2 * pixels
            p_ac = acc[:XBLOCK, first : first + pixels]
            p_ad = acc[:XBLOCK, first + pixels : first + 2 * pixels]
            p_bc = acc[XBLOCK:, first : first + pixels]
            p_bd = acc[XBLOCK:, first + pixels : first + 2 * pixels]
            cos_part, sin_part = turn_cos_sin(depth_ref[item] * depth)
            if block == 0:
                top = x_row == 0
                top_cos, top_sin = turn_cos_sin(depth_ref[item] * top_depth)
                top_value = p_bc * top_cos - p_bd * top_sin
                p_bc = jnp.where(top, 0.0, p_bc)
                p_bd = jnp.where(top, 0.0, p_bd)
            above += (p_ac - p_bd) * cos_part - (p_ad + p_bc) * sin_part
            lower = (p_ac + p_bd) * cos_part - (p_ad - p_bc) * sin_part
            if block == 0:
                lower = jnp.where(top, top_value, lower)
            below += lower
        part, sub = block // subs, block % subs
        rows = slice(sub * XBLOCK, (sub + 1) * XBLOCK)
        for owner, value in ((part, above), (blocks - 1 - part, below)):
            image[owner, rows, :] = value

            @pl.when(me_wa != owner)
            def _():
                image_copy(owner, sub).start()

        if sub == 0:
            target = blocks - 1 - (part - 1) % parts
            tail[target, 1:2, :] = below[0:1]

    tail_copies = [tail_copy(step) for step in range(1, blocks)]
    start_all(tail_copies)
    total = image[me_wa]
    total_tail = tail[me_wa]
    for step in range(1, blocks):
        for sub in range(subs):
            rows = pl.ds(sub * XBLOCK, XBLOCK)
            pltpu.make_async_remote_copy(
                src_ref=image.at[me_wa, rows],
                dst_ref=held.at[step - 1, rows],
                send_sem=image_send.at[me_wa, sub],
                recv_sem=image_recv.at[step - 1, sub],
                device_id={"wa": lax.rem(me_wa + step, blocks)},
                device_id_type=MESH,
            ).wait_recv()
        total = total + held[step - 1]
    for step, copy in enumerate(tail_copies):
        copy.wait()
        total_tail = total_tail + held_tail[step]
    scale = 1.0 / jnp.sqrt(total_tail[0:1])
    out_row = lax.broadcasted_iota(jnp.int32, (chunk_rows, chunk_rows), 0)
    in_row = lax.broadcasted_iota(jnp.int32, (chunk_rows, chunk_rows), 1)
    mirrored = me_wa * 2 >= blocks
    turned = jnp.where(mirrored, (chunk_rows - out_row) % chunk_rows, out_row)
    chosen = jnp.where(turned == in_row, 1.0, 0.0).astype(jnp.bfloat16)
    high, rest = split(total)
    low, last = split(total - high.astype(jnp.float32))
    ordered = sum(
        jnp.dot(chosen, piece, preferred_element_type=jnp.float32) for piece in (high, low, last)
    )
    out_line = lax.broadcasted_iota(jnp.int32, (chunk_rows, 1), 0)
    swap = jnp.where(mirrored, out_line, 1) == 0
    out_ref[...] = jnp.where(swap, total_tail[1:2], ordered) * scale
    for owner in range(blocks):

        @pl.when(me_wa != owner)
        def _():
            for sub in range(subs):
                image_copy(owner, sub).wait_send()


def body(
    visibilities,
    weights,
    cell_index,
    kernel_index,
    layer_index,
    tile_counts,
    kernel_table,
    layer_depth,
):
    layer_dev = layer_depth.shape[0]
    peers = lax.axis_size("bl")
    blocks = lax.axis_size("wa")
    pixels = GRID // peers
    chunk_rows = GRID // blocks
    own_tiles = cell_index.shape[1]
    tiles = peers * own_tiles
    count = tiles * LANES
    half = GRID // 2
    columns = 2 * layer_dev * pixels
    vmem = pl.BlockSpec(memory_space=pltpu.VMEM)
    anywhere = pl.BlockSpec(memory_space=pltpu.HBM)
    f32, bf16 = jnp.float32, jnp.bfloat16
    shapes = [
        ((own_tiles, 8, LANES), f32),
        ((tiles, 8, LANES), f32),
        ((LANES, LANES), f32),
        ((half, LANES), f32),
        ((half, LANES), f32),
        ((pixels, LANES), f32),
        ((pixels, LANES), f32),
        ((FINE, count), f32),
        ((FINE, count), f32),
        ((half // FINE, count), f32),
        ((half // FINE, count), f32),
        ((columns, PIECES * count), bf16),
        ((2, 2 * XBLOCK, PIECES * count), bf16),
        ((2 * XBLOCK, columns), f32),
        ((blocks, chunk_rows, pixels), f32),
        ((blocks, 8, pixels), f32),
        ((blocks - 1, chunk_rows, pixels), f32),
        ((blocks - 1, 8, pixels), f32),
    ]
    subs = chunk_rows // XBLOCK
    semaphores = [
        (peers - 1,),
        (peers - 1,),
        (blocks, subs),
        (blocks - 1, subs),
        (blocks - 1,),
        (blocks - 1,),
    ]
    return pl.pallas_call(
        functools.partial(kernel, layer_dev, pixels, blocks, peers),
        out_shape=jax.ShapeDtypeStruct((chunk_rows, pixels), f32),
        in_specs=[anywhere] * 8,
        out_specs=vmem,
        scratch_shapes=[pltpu.SMEM(layer_depth.shape, f32)]
        + [
            pltpu.VMEM(value.shape, value.dtype)
            for value in (
                tile_counts,
                kernel_table.T,
                visibilities,
                weights,
                cell_index,
                kernel_index,
                layer_index,
            )
        ]
        + [pltpu.SemaphoreType.DMA((8,))]
        + [pltpu.VMEM(shape, kind) for shape, kind in shapes]
        + [pltpu.SemaphoreType.DMA(shape) for shape in semaphores],
        compiler_params=pltpu.CompilerParams(
            collective_id=0, has_side_effects=True, vmem_limit_bytes=67043328
        ),
        name="dirty_image",
    )(
        layer_depth,
        tile_counts,
        kernel_table.T,
        visibilities,
        weights,
        cell_index,
        kernel_index,
        layer_index,
    )


def solution(mesh):
    in_specs = (
        P("wa", "bl", None, None),
        P("wa", "bl", None),
        P("wa", "bl", None),
        P("wa", "bl", None),
        P("wa", "bl", None),
        P("wa", "bl"),
        P(),
        P("wa"),
    )
    out_specs = P("wa", "bl")
    return jax.shard_map(body, mesh=mesh, in_specs=in_specs, out_specs=out_specs, check_vma=False)
```

```python
import functools
import math

import jax
import jax.numpy as jnp
from jax import lax
from jax.experimental import pallas as pl
from jax.experimental.pallas import tpu as pltpu
from jax.sharding import PartitionSpec as P

GRID = 1024
SUPPORT = 8
OVERSAMPLE = 16
LANES = 128
FINE = 32
XBLOCK = 128
CHUNK = 2 * LANES
PIECES = 3

field_of_view = 0.6
MESH = pl.DeviceIdType.MESH

TWO_PI = 2.0 * math.pi
SIN_TERMS = [(-1) ** k * TWO_PI ** (2 * k + 1) / math.factorial(2 * k + 1) for k in range(9)]
COS_TERMS = [(-1) ** k * TWO_PI ** (2 * k) / math.factorial(2 * k) for k in range(10)]


def horner(square, terms):
    value = jnp.full_like(square, terms[-1])
    for term in terms[-2::-1]:
        value = value * square + term
    return value


def turn_cos_sin(turns):
    part = turns - jnp.round(turns)
    square = part * part
    return horner(square, COS_TERMS), part * horner(square, SIN_TERMS)


def split(value):
    high = value.astype(jnp.bfloat16)
    return high, (value - high.astype(jnp.float32)).astype(jnp.bfloat16)


def dot_nt(a, b):
    return lax.dot_general(
        a, b, (((1,), (1,)), ((), ())), preferred_element_type=jnp.float32
    )


def factor_table(first, rows, table, special):
    pixel = (first + lax.broadcasted_iota(jnp.int32, (rows, LANES), 0)).astype(jnp.float32)
    offset_lane = lax.broadcasted_iota(jnp.int32, (rows, LANES), 1)
    offset = (offset_lane % SUPPORT - SUPPORT // 2).astype(jnp.float32)
    cos_part, sin_part = turn_cos_sin(pixel * offset * (1.0 / GRID))
    if special:
        row = lax.broadcasted_iota(jnp.int32, (rows, LANES), 0)
        parity = 1.0 - 2.0 * (offset_lane % 2).astype(jnp.float32)
        sin_part = jnp.where(row == 0, parity, sin_part)
    table_high, table_low = split(table)

    def product(part):
        high, low = split(part)
        return dot_nn(high, table_high) + dot_nn(high, table_low) + dot_nn(low, table_high)

    return product(cos_part), product(sin_part)


def dot_nn(a, b):
    return jnp.dot(a, b, preferred_element_type=jnp.float32)


def start_all(copies):
    for copy in copies:
        copy.start()


def kernel(
    layer_dev,
    pixels,
    blocks,
    peers,
    depth_hbm,
    counts_hbm,
    table_hbm,
    vis_hbm,
    weight_hbm,
    cell_hbm,
    index_hbm,
    layer_hbm,
    out_ref,
    depth_ref,
    counts_ref,
    table_ref,
    vis_ref,
    weight_ref,
    cell_ref,
    index_ref,
    layer_ref,
    load_sem,
    own,
    slots_ref,
    table_pad,
    u_re,
    u_im,
    v_re,
    v_im,
    fine_re,
    fine_im,
    coarse_re,
    coarse_im,
    rhs,
    lhs_even,
    lhs_odd,
    rhs_even,
    rhs_odd,
    acc,
    image,
    tail,
    held,
    held_tail,
    slot_send,
    slot_recv,
    image_send,
    image_recv,
    tail_send,
    tail_recv,
):
    half = GRID // 2
    chunk_rows = GRID // blocks
    own_tiles = own.shape[0]
    tiles = peers * own_tiles
    block_total = half // XBLOCK
    subs = chunk_rows // XBLOCK
    block_groups = XBLOCK // FINE
    me_bl, me_wa = lax.axis_index("bl"), lax.axis_index("wa")
    loads = [
        pltpu.make_async_copy(source, target, load_sem.at[place])
        for place, (source, target) in enumerate(
            (
                (counts_hbm, counts_ref),
                (vis_hbm, vis_ref),
                (weight_hbm, weight_ref),
                (cell_hbm, cell_ref),
                (index_hbm, index_ref),
                (layer_hbm, layer_ref),
                (table_hbm, table_ref),
                (depth_hbm, depth_ref),
            )
        )
    ]
    start_all(loads)
    barrier = pltpu.get_barrier_semaphore()
    for axis, me, count in (("bl", me_bl, peers), ("wa", me_wa, blocks)):
        for step in range(1, count):
            pl.semaphore_signal(
                barrier, inc=1, device_id={axis: lax.rem(me + step, count)}, device_id_type=MESH
            )
    for load in loads:
        load.wait()
    position = lax.broadcasted_iota(jnp.int32, (1, LANES), 1)
    for tile in range(own_tiles):
        line = slice(tile, tile + 1)
        weight = jnp.where(position < counts_ref[0:1, tile : tile + 1], weight_ref[0, line], 0.0)
        cell, index = cell_ref[0, line], index_ref[0, line]
        values = [
            vis_ref[0, tile, 0:1] * weight,
            vis_ref[0, tile, 1:2] * weight,
            weight,
            (cell // GRID).astype(jnp.float32),
            (cell % GRID).astype(jnp.float32),
            (index // OVERSAMPLE).astype(jnp.float32),
            (index % OVERSAMPLE).astype(jnp.float32),
            layer_ref[0, line].astype(jnp.float32),
        ]
        for place, value in enumerate(values):
            own[tile, place : place + 1] = value
    pl.semaphore_wait(barrier, peers + blocks - 2)
    slot_copies = [
        pltpu.make_async_remote_copy(
            src_ref=own,
            dst_ref=slots_ref.at[pl.ds(me_bl * own_tiles, own_tiles)],
            send_sem=slot_send.at[step - 1],
            recv_sem=slot_recv.at[step - 1],
            device_id={"bl": lax.rem(me_bl + step, peers)},
            device_id_type=MESH,
        )
        for step in range(1, peers)
    ]
    start_all(slot_copies)
    slots_ref[pl.ds(me_bl * own_tiles, own_tiles)] = own[...]

    first_pixel = me_bl * pixels
    table_pad[...] = jnp.zeros_like(table_pad)
    table_pad[0:SUPPORT, 0:OVERSAMPLE] = table_ref[...]
    table = table_pad[...]
    u_re[...], u_im[...] = factor_table(0, half, table, True)
    v_re[...], v_im[...] = factor_table(first_pixel, pixels, table, False)
    fine_x = lax.broadcasted_iota(jnp.int32, (FINE, LANES), 0).astype(jnp.float32)
    coarse_x = (lax.broadcasted_iota(jnp.int32, (half // FINE, LANES), 0) * FINE).astype(
        jnp.float32
    )
    pixel_y = (
        first_pixel + lax.broadcasted_iota(jnp.int32, (pixels // FINE, LANES), 0) * FINE
    ).astype(jnp.float32)
    for copy in slot_copies:
        copy.wait()

    def lanes_of(tile):
        return pl.ds(pl.multiple_of(tile * LANES, LANES), LANES)

    def piece_lanes(tile):
        base = tile // 2 * (PIECES * CHUNK) + tile % 2 * LANES
        return [
            pl.ds(pl.multiple_of(base + piece * CHUNK, LANES), LANES) for piece in range(PIECES)
        ]

    def stage_lanes(part_of_chunk):
        starts = [piece * CHUNK + part_of_chunk * LANES for piece in range(PIECES)]
        return [slice(start, start + LANES) for start in starts]

    def prepare(tile, stage, part_of_chunk):
        lanes = lanes_of(tile)
        places = piece_lanes(tile)
        staged = stage_lanes(part_of_chunk)
        params = slots_ref[tile]
        vis_real, vis_imag = params[0:1], params[1:2]
        row, col = params[3:4] * (1.0 / GRID), params[4:5] * (1.0 / GRID)
        col_kernel = params[6:7].astype(jnp.int32)
        layer = params[7:8]
        fine_re[:, lanes], fine_im[:, lanes] = turn_cos_sin(row * fine_x)
        cx_re, cx_im = turn_cos_sin(row * coarse_x)
        for block in range(block_total):
            lines = slice(block * block_groups, (block + 1) * block_groups)
            coarse_re[block, :, lanes] = cx_re[lines]
            coarse_im[block, :, lanes] = cx_im[lines]
        cf_re, cf_im = turn_cos_sin(col * fine_x)
        cc_re, cc_im = turn_cos_sin(col * pixel_y)
        cv_re = cc_re * vis_real - cc_im * vis_imag
        cv_im = cc_re * vis_imag + cc_im * vis_real
        masks = [
            jnp.broadcast_to(jnp.where(layer == float(item), 1.0, 0.0), (FINE, LANES))
            for item in range(layer_dev)
        ]
        index = jnp.broadcast_to(col_kernel, (FINE, LANES))
        for group in range(pixels // FINE):
            rows = slice(group * FINE, (group + 1) * FINE)
            k_re = jnp.take_along_axis(v_re[rows, :], index, axis=1, mode="promise_in_bounds")
            k_im = jnp.take_along_axis(v_im[rows, :], index, axis=1, mode="promise_in_bounds")
            e_re = cf_re * cv_re[group : group + 1] - cf_im * cv_im[group : group + 1]
            e_im = cf_re * cv_im[group : group + 1] + cf_im * cv_re[group : group + 1]
            real = e_re * k_re - e_im * k_im
            imag = e_re * k_im + e_im * k_re
            for item in range(layer_dev):
                for place, value in enumerate((real, imag)):
                    high, low = split(value * masks[item])
                    start = (item * 2 + place) * pixels + group * FINE
                    for where, near, piece in zip(places, staged, (high, low, high)):
                        rhs[start : start + FINE, where] = piece
                        stage[start : start + FINE, near] = piece

    square_sum = jnp.sum(slots_ref[:, 2:3, :] * slots_ref[:, 2:3, :])

    def expand(block, side, tile, part_of_chunk):
        lanes = lanes_of(tile)
        places = stage_lanes(part_of_chunk)
        params = slots_ref[tile]
        index = jnp.broadcast_to(params[5:6].astype(jnp.int32), (FINE, LANES))
        f_re, f_im = fine_re[:, lanes], fine_im[:, lanes]
        c_re, c_im = coarse_re[block, :, lanes], coarse_im[block, :, lanes]
        for group in range(XBLOCK // FINE):
            place = block * (XBLOCK // FINE) + group
            rows = pl.ds(pl.multiple_of(place * FINE, FINE), FINE)
            k_re = jnp.take_along_axis(u_re[rows, :], index, axis=1, mode="promise_in_bounds")
            k_im = jnp.take_along_axis(u_im[rows, :], index, axis=1, mode="promise_in_bounds")
            g_re, g_im = c_re[group : group + 1], c_im[group : group + 1]
            e_re = f_re * g_re - f_im * g_im
            e_im = f_re * g_im + f_im * g_re
            real = e_re * k_re - e_im * k_im
            imag = e_re * k_im + e_im * k_re
            if group == 0:
                odd = params[3:4].astype(jnp.int32) % 2
                sign = (1 - 2 * odd).astype(jnp.float32)
                first_row = lax.broadcasted_iota(jnp.int32, (FINE, LANES), 0) == 0
                imag = imag * jnp.where(first_row & (block == 0), sign, 1.0)
            for part, value in enumerate((real, imag)):
                high, low = split(value)
                start = part * XBLOCK + group * FINE
                for where, piece in zip(places, (high, high, low)):
                    side[start : start + FINE, where] = piece

    def image_copy(owner, sub):
        slot = lax.rem(owner - me_wa + blocks, blocks) - 1
        rows = pl.ds(sub * XBLOCK, XBLOCK)
        return pltpu.make_async_remote_copy(
            src_ref=image.at[owner, rows],
            dst_ref=held.at[slot, rows],
            send_sem=image_send.at[owner, sub],
            recv_sem=image_recv.at[slot, sub],
            device_id={"wa": owner},
            device_id_type=MESH,
        )

    def tail_copy(step):
        peer = lax.rem(me_wa + step, blocks)
        return pltpu.make_async_remote_copy(
            src_ref=tail.at[peer],
            dst_ref=held_tail.at[step - 1],
            send_sem=tail_send.at[step - 1],
            recv_sem=tail_recv.at[step - 1],
            device_id={"wa": peer},
            device_id_type=MESH,
        )

    y_pixel = first_pixel + lax.broadcasted_iota(jnp.int32, (1, pixels), 1)
    y_coord = (y_pixel - GRID // 2).astype(jnp.float32) * (field_of_view / GRID)
    top_depth = jnp.sqrt(1.0 - y_coord * y_coord) - 1.0
    tail[...] = jnp.full_like(tail, square_sum)

    chunks = tiles // 2
    lhs_sides, rhs_sides = (lhs_even, lhs_odd), (rhs_even, rhs_odd)
    for part_of_chunk in range(2):
        prepare(part_of_chunk, rhs_even, part_of_chunk)
        expand(0, lhs_even, part_of_chunk, part_of_chunk)

    parts = blocks // 2
    order = [first + part * subs for first in range(subs) for part in range(block_total // subs)]
    for turn, block in enumerate(order):
        following = order[turn + 1] if turn + 1 < block_total else block

        @pl.loop(0, chunks // 2)
        def _(couple):
            total = jnp.where(couple == 0, 0.0, acc[...])
            for parity in range(2):
                chunk = couple * 2 + parity
                wide = pl.ds(pl.multiple_of(chunk * (PIECES * CHUNK), LANES), PIECES * CHUNK)
                right = rhs[:, wide] if turn else rhs_sides[parity][...]
                total = total + dot_nt(lhs_sides[parity][...], right)
                coming = lax.rem(chunk + 1, chunks)
                coming_block = jnp.where(coming == 0, following, block)
                for part_of_chunk in range(2):
                    tile = coming * 2 + part_of_chunk
                    if turn == 0:
                        prepare(tile, rhs_sides[1 - parity], part_of_chunk)
                    expand(coming_block, lhs_sides[1 - parity], tile, part_of_chunk)
            acc[...] = total

        x_row = block * XBLOCK + lax.broadcasted_iota(jnp.int32, (XBLOCK, 1), 0)
        x_coord = (x_row - GRID // 2).astype(jnp.float32) * (field_of_view / GRID)
        depth = jnp.sqrt(1.0 - x_coord * x_coord - y_coord * y_coord) - 1.0
        above = jnp.zeros((XBLOCK, pixels), jnp.float32)
        below = jnp.zeros((XBLOCK, pixels), jnp.float32)
        for item in range(layer_dev):
            first = item * 2 * pixels
            p_ac = acc[:XBLOCK, first : first + pixels]
            p_ad = acc[:XBLOCK, first + pixels : first + 2 * pixels]
            p_bc = acc[XBLOCK:, first : first + pixels]
            p_bd = acc[XBLOCK:, first + pixels : first + 2 * pixels]
            cos_part, sin_part = turn_cos_sin(depth_ref[item] * depth)
            if block == 0:
                top = x_row == 0
                top_cos, top_sin = turn_cos_sin(depth_ref[item] * top_depth)
                top_value = p_bc * top_cos - p_bd * top_sin
                p_bc = jnp.where(top, 0.0, p_bc)
                p_bd = jnp.where(top, 0.0, p_bd)
            above += (p_ac - p_bd) * cos_part - (p_ad + p_bc) * sin_part
            lower = (p_ac + p_bd) * cos_part - (p_ad - p_bc) * sin_part
            if block == 0:
                lower = jnp.where(top, top_value, lower)
            below += lower
        part, sub = block // subs, block % subs
        rows = slice(sub * XBLOCK, (sub + 1) * XBLOCK)
        for owner, value in ((part, above), (blocks - 1 - part, below)):
            image[owner, rows, :] = value

            @pl.when(me_wa != owner)
            def _():
                image_copy(owner, sub).start()

        if sub == 0:
            target = blocks - 1 - (part - 1) % parts
            tail[target, 1:2, :] = below[0:1]

    tail_copies = [tail_copy(step) for step in range(1, blocks)]
    start_all(tail_copies)
    total = image[me_wa]
    total_tail = tail[me_wa]
    for step in range(1, blocks):
        for sub in range(subs):
            rows = pl.ds(sub * XBLOCK, XBLOCK)
            pltpu.make_async_remote_copy(
                src_ref=image.at[me_wa, rows],
                dst_ref=held.at[step - 1, rows],
                send_sem=image_send.at[me_wa, sub],
                recv_sem=image_recv.at[step - 1, sub],
                device_id={"wa": lax.rem(me_wa + step, blocks)},
                device_id_type=MESH,
            ).wait_recv()
        total = total + held[step - 1]
    for step, copy in enumerate(tail_copies):
        copy.wait()
        total_tail = total_tail + held_tail[step]
    scale = 1.0 / jnp.sqrt(total_tail[0:1])
    out_row = lax.broadcasted_iota(jnp.int32, (chunk_rows, chunk_rows), 0)
    in_row = lax.broadcasted_iota(jnp.int32, (chunk_rows, chunk_rows), 1)
    mirrored = me_wa * 2 >= blocks
    turned = jnp.where(mirrored, (chunk_rows - out_row) % chunk_rows, out_row)
    chosen = jnp.where(turned == in_row, 1.0, 0.0).astype(jnp.bfloat16)
    high, rest = split(total)
    low, last = split(total - high.astype(jnp.float32))
    ordered = sum(
        jnp.dot(chosen, piece, preferred_element_type=jnp.float32) for piece in (high, low, last)
    )
    out_line = lax.broadcasted_iota(jnp.int32, (chunk_rows, 1), 0)
    swap = jnp.where(mirrored, out_line, 1) == 0
    out_ref[...] = jnp.where(swap, total_tail[1:2], ordered) * scale
    for owner in range(blocks):

        @pl.when(me_wa != owner)
        def _():
            for sub in range(subs):
                image_copy(owner, sub).wait_send()


def body(
    visibilities,
    weights,
    cell_index,
    kernel_index,
    layer_index,
    tile_counts,
    kernel_table,
    layer_depth,
):
    layer_dev = layer_depth.shape[0]
    peers = lax.axis_size("bl")
    blocks = lax.axis_size("wa")
    pixels = GRID // peers
    chunk_rows = GRID // blocks
    own_tiles = cell_index.shape[1]
    tiles = peers * own_tiles
    count = tiles * LANES
    half = GRID // 2
    columns = 2 * layer_dev * pixels
    vmem = pl.BlockSpec(memory_space=pltpu.VMEM)
    anywhere = pl.BlockSpec(memory_space=pltpu.HBM)
    f32, bf16 = jnp.float32, jnp.bfloat16
    shapes = [
        ((own_tiles, 8, LANES), f32),
        ((tiles, 8, LANES), f32),
        ((LANES, LANES), f32),
        ((half, LANES), f32),
        ((half, LANES), f32),
        ((pixels, LANES), f32),
        ((pixels, LANES), f32),
        ((FINE, count), f32),
        ((FINE, count), f32),
        ((half // XBLOCK, XBLOCK // FINE, count), f32),
        ((half // XBLOCK, XBLOCK // FINE, count), f32),
        ((columns, PIECES * count), bf16),
        ((2 * XBLOCK, PIECES * CHUNK), bf16),
        ((2 * XBLOCK, PIECES * CHUNK), bf16),
        ((columns, PIECES * CHUNK), bf16),
        ((columns, PIECES * CHUNK), bf16),
        ((2 * XBLOCK, columns), f32),
        ((blocks, chunk_rows, pixels), f32),
        ((blocks, 8, pixels), f32),
        ((blocks - 1, chunk_rows, pixels), f32),
        ((blocks - 1, 8, pixels), f32),
    ]
    subs = chunk_rows // XBLOCK
    semaphores = [
        (peers - 1,),
        (peers - 1,),
        (blocks, subs),
        (blocks - 1, subs),
        (blocks - 1,),
        (blocks - 1,),
    ]
    return pl.pallas_call(
        functools.partial(kernel, layer_dev, pixels, blocks, peers),
        out_shape=jax.ShapeDtypeStruct((chunk_rows, pixels), f32),
        in_specs=[anywhere] * 8,
        out_specs=vmem,
        scratch_shapes=[pltpu.SMEM(layer_depth.shape, f32)]
        + [
            pltpu.VMEM(value.shape, value.dtype)
            for value in (
                tile_counts,
                kernel_table.T,
                visibilities,
                weights,
                cell_index,
                kernel_index,
                layer_index,
            )
        ]
        + [pltpu.SemaphoreType.DMA((8,))]
        + [pltpu.VMEM(shape, kind) for shape, kind in shapes]
        + [pltpu.SemaphoreType.DMA(shape) for shape in semaphores],
        compiler_params=pltpu.CompilerParams(
            collective_id=0, has_side_effects=True, vmem_limit_bytes=48 * 1024 * 1024
        ),
        name="dirty_image",
    )(
        layer_depth,
        tile_counts,
        kernel_table.T,
        visibilities,
        weights,
        cell_index,
        kernel_index,
        layer_index,
    )


def solution(mesh):
    in_specs = (
        P("wa", "bl", None, None),
        P("wa", "bl", None),
        P("wa", "bl", None),
        P("wa", "bl", None),
        P("wa", "bl", None),
        P("wa", "bl"),
        P(),
        P("wa"),
    )
    out_specs = P("wa", "bl")
    return jax.shard_map(body, mesh=mesh, in_specs=in_specs, out_specs=out_specs, check_vma=False)
```

```python
import functools
import math

import jax
import jax.numpy as jnp
from jax import lax
from jax.experimental import pallas as pl
from jax.experimental.pallas import tpu as pltpu
from jax.sharding import PartitionSpec as P

GRID = 1024
SUPPORT = 8
OVERSAMPLE = 16
LANES = 128
FINE = 32
XBLOCK = 128
CHUNK = 2 * LANES
PIECES = 3

field_of_view = 0.6
MESH = pl.DeviceIdType.MESH

TWO_PI = 2.0 * math.pi
SIN_TERMS = [(-1) ** k * TWO_PI ** (2 * k + 1) / math.factorial(2 * k + 1) for k in range(8)]
COS_TERMS = [(-1) ** k * TWO_PI ** (2 * k) / math.factorial(2 * k) for k in range(9)]


def horner(square, terms):
    value = jnp.full_like(square, terms[-1])
    for term in terms[-2::-1]:
        value = value * square + term
    return value


def turn_cos_sin(turns):
    part = turns - jnp.round(turns)
    square = part * part
    return horner(square, COS_TERMS), part * horner(square, SIN_TERMS)


def split(value):
    high = value.astype(jnp.bfloat16)
    return high, (value - high.astype(jnp.float32)).astype(jnp.bfloat16)


def dot_nt(a, b):
    return lax.dot_general(
        a, b, (((1,), (1,)), ((), ())), preferred_element_type=jnp.float32
    )


def factor_table(first, rows, table, special):
    pixel = (first + lax.broadcasted_iota(jnp.int32, (rows, LANES), 0)).astype(jnp.float32)
    offset_lane = lax.broadcasted_iota(jnp.int32, (rows, LANES), 1)
    offset = (offset_lane % SUPPORT - SUPPORT // 2).astype(jnp.float32)
    cos_part, sin_part = turn_cos_sin(pixel * offset * (1.0 / GRID))
    if special:
        row = lax.broadcasted_iota(jnp.int32, (rows, LANES), 0)
        parity = 1.0 - 2.0 * (offset_lane % 2).astype(jnp.float32)
        sin_part = jnp.where(row == 0, parity, sin_part)
    table_high, table_low = split(table)

    def product(part):
        high, low = split(part)
        return dot_nt(high, table_high) + dot_nt(high, table_low) + dot_nt(low, table_high)

    return product(cos_part), product(sin_part)


def start_all(copies):
    for copy in copies:
        copy.start()


def kernel(
    layer_dev,
    pixels,
    blocks,
    peers,
    depth_ref,
    counts_ref,
    table_ref,
    vis_ref,
    weight_ref,
    cell_ref,
    index_ref,
    layer_ref,
    out_ref,
    own,
    slots_ref,
    table_pad,
    u_re,
    u_im,
    v_re,
    v_im,
    fine_re,
    fine_im,
    coarse_re,
    coarse_im,
    rhs,
    lhs_even,
    lhs_odd,
    rhs_even,
    rhs_odd,
    acc,
    image,
    tail,
    held,
    held_tail,
    slot_send,
    slot_recv,
    image_send,
    image_recv,
    tail_send,
    tail_recv,
):
    half = GRID // 2
    chunk_rows = GRID // blocks
    own_tiles = own.shape[0]
    tiles = peers * own_tiles
    block_total = half // XBLOCK
    subs = chunk_rows // XBLOCK
    block_groups = XBLOCK // FINE
    me_bl, me_wa = lax.axis_index("bl"), lax.axis_index("wa")
    barrier = pltpu.get_barrier_semaphore()
    for axis, me, count in (("bl", me_bl, peers), ("wa", me_wa, blocks)):
        for step in range(1, count):
            pl.semaphore_signal(
                barrier, inc=1, device_id={axis: lax.rem(me + step, count)}, device_id_type=MESH
            )
    position = lax.broadcasted_iota(jnp.int32, (1, LANES), 1)
    for tile in range(own_tiles):
        line = slice(tile, tile + 1)
        weight = jnp.where(position < counts_ref[0, tile], weight_ref[0, line], 0.0)
        cell, index = cell_ref[0, line], index_ref[0, line]
        values = [
            vis_ref[0, tile, 0:1] * weight,
            vis_ref[0, tile, 1:2] * weight,
            weight,
            (cell // GRID).astype(jnp.float32),
            (cell % GRID).astype(jnp.float32),
            (index // OVERSAMPLE).astype(jnp.float32),
            (index % OVERSAMPLE).astype(jnp.float32),
            layer_ref[0, line].astype(jnp.float32),
        ]
        for place, value in enumerate(values):
            own[tile, place : place + 1] = value
    pl.semaphore_wait(barrier, peers + blocks - 2)
    slot_copies = [
        pltpu.make_async_remote_copy(
            src_ref=own,
            dst_ref=slots_ref.at[pl.ds(me_bl * own_tiles, own_tiles)],
            send_sem=slot_send.at[step - 1],
            recv_sem=slot_recv.at[step - 1],
            device_id={"bl": lax.rem(me_bl + step, peers)},
            device_id_type=MESH,
        )
        for step in range(1, peers)
    ]
    start_all(slot_copies)
    slots_ref[pl.ds(me_bl * own_tiles, own_tiles)] = own[...]

    first_pixel = me_bl * pixels
    table_pad[...] = jnp.zeros_like(table_pad)
    table_pad[0:OVERSAMPLE, 0:SUPPORT] = table_ref[...]
    table = table_pad[...]
    u_re[...], u_im[...] = factor_table(0, half, table, True)
    v_re[...], v_im[...] = factor_table(first_pixel, pixels, table, False)
    fine_x = lax.broadcasted_iota(jnp.int32, (FINE, LANES), 0).astype(jnp.float32)
    coarse_x = (lax.broadcasted_iota(jnp.int32, (half // FINE, LANES), 0) * FINE).astype(
        jnp.float32
    )
    pixel_y = (
        first_pixel + lax.broadcasted_iota(jnp.int32, (pixels // FINE, LANES), 0) * FINE
    ).astype(jnp.float32)
    for copy in slot_copies:
        copy.wait()

    def lanes_of(tile):
        return pl.ds(pl.multiple_of(tile * LANES, LANES), LANES)

    def piece_lanes(tile):
        base = tile // 2 * (PIECES * CHUNK) + tile % 2 * LANES
        return [
            pl.ds(pl.multiple_of(base + piece * CHUNK, LANES), LANES) for piece in range(PIECES)
        ]

    def stage_lanes(part_of_chunk):
        starts = [piece * CHUNK + part_of_chunk * LANES for piece in range(PIECES)]
        return [slice(start, start + LANES) for start in starts]

    def prepare(tile, stage, part_of_chunk):
        lanes = lanes_of(tile)
        places = piece_lanes(tile)
        staged = stage_lanes(part_of_chunk)
        params = slots_ref[tile]
        vis_real, vis_imag = params[0:1], params[1:2]
        row, col = params[3:4] * (1.0 / GRID), params[4:5] * (1.0 / GRID)
        col_kernel = params[6:7].astype(jnp.int32)
        layer = params[7:8]
        fine_re[:, lanes], fine_im[:, lanes] = turn_cos_sin(row * fine_x)
        cx_re, cx_im = turn_cos_sin(row * coarse_x)
        for block in range(block_total):
            lines = slice(block * block_groups, (block + 1) * block_groups)
            coarse_re[block, :, lanes] = cx_re[lines]
            coarse_im[block, :, lanes] = cx_im[lines]
        cf_re, cf_im = turn_cos_sin(col * fine_x)
        cc_re, cc_im = turn_cos_sin(col * pixel_y)
        cv_re = cc_re * vis_real - cc_im * vis_imag
        cv_im = cc_re * vis_imag + cc_im * vis_real
        masks = [
            jnp.broadcast_to(jnp.where(layer == float(item), 1.0, 0.0), (FINE, LANES))
            for item in range(layer_dev)
        ]
        index = jnp.broadcast_to(col_kernel, (FINE, LANES))
        for group in range(pixels // FINE):
            rows = slice(group * FINE, (group + 1) * FINE)
            k_re = jnp.take_along_axis(v_re[rows, :], index, axis=1, mode="promise_in_bounds")
            k_im = jnp.take_along_axis(v_im[rows, :], index, axis=1, mode="promise_in_bounds")
            e_re = cf_re * cv_re[group : group + 1] - cf_im * cv_im[group : group + 1]
            e_im = cf_re * cv_im[group : group + 1] + cf_im * cv_re[group : group + 1]
            real = e_re * k_re - e_im * k_im
            imag = e_re * k_im + e_im * k_re
            for item in range(layer_dev):
                for place, value in enumerate((real, imag)):
                    high, low = split(value * masks[item])
                    start = (item * 2 + place) * pixels + group * FINE
                    for where, near, piece in zip(places, staged, (high, low, high)):
                        rhs[start : start + FINE, where] = piece
                        stage[start : start + FINE, near] = piece

    square_sum = jnp.sum(slots_ref[:, 2:3, :] * slots_ref[:, 2:3, :])

    def expand(block, side, tile, part_of_chunk):
        lanes = lanes_of(tile)
        places = stage_lanes(part_of_chunk)
        params = slots_ref[tile]
        index = jnp.broadcast_to(params[5:6].astype(jnp.int32), (FINE, LANES))
        f_re, f_im = fine_re[:, lanes], fine_im[:, lanes]
        c_re, c_im = coarse_re[block, :, lanes], coarse_im[block, :, lanes]
        for group in range(XBLOCK // FINE):
            place = block * (XBLOCK // FINE) + group
            rows = pl.ds(pl.multiple_of(place * FINE, FINE), FINE)
            k_re = jnp.take_along_axis(u_re[rows, :], index, axis=1, mode="promise_in_bounds")
            k_im = jnp.take_along_axis(u_im[rows, :], index, axis=1, mode="promise_in_bounds")
            g_re, g_im = c_re[group : group + 1], c_im[group : group + 1]
            e_re = f_re * g_re - f_im * g_im
            e_im = f_re * g_im + f_im * g_re
            real = e_re * k_re - e_im * k_im
            imag = e_re * k_im + e_im * k_re
            if group == 0:
                odd = params[3:4].astype(jnp.int32) % 2
                sign = (1 - 2 * odd).astype(jnp.float32)
                first_row = lax.broadcasted_iota(jnp.int32, (FINE, LANES), 0) == 0
                imag = imag * jnp.where(first_row & (block == 0), sign, 1.0)
            for part, value in enumerate((real, imag)):
                high, low = split(value)
                start = part * XBLOCK + group * FINE
                for where, piece in zip(places, (high, high, low)):
                    side[start : start + FINE, where] = piece

    def image_copy(owner, sub):
        slot = lax.rem(owner - me_wa + blocks, blocks) - 1
        rows = pl.ds(sub * XBLOCK, XBLOCK)
        return pltpu.make_async_remote_copy(
            src_ref=image.at[owner, rows],
            dst_ref=held.at[slot, rows],
            send_sem=image_send.at[owner, sub],
            recv_sem=image_recv.at[slot, sub],
            device_id={"wa": owner},
            device_id_type=MESH,
        )

    def tail_copy(step):
        peer = lax.rem(me_wa + step, blocks)
        return pltpu.make_async_remote_copy(
            src_ref=tail.at[peer],
            dst_ref=held_tail.at[step - 1],
            send_sem=tail_send.at[step - 1],
            recv_sem=tail_recv.at[step - 1],
            device_id={"wa": peer},
            device_id_type=MESH,
        )

    y_pixel = first_pixel + lax.broadcasted_iota(jnp.int32, (1, pixels), 1)
    y_coord = (y_pixel - GRID // 2).astype(jnp.float32) * (field_of_view / GRID)
    top_depth = jnp.sqrt(1.0 - y_coord * y_coord) - 1.0
    tail[...] = jnp.full_like(tail, square_sum)

    chunks = tiles // 2
    lhs_sides, rhs_sides = (lhs_even, lhs_odd), (rhs_even, rhs_odd)
    for part_of_chunk in range(2):
        prepare(part_of_chunk, rhs_even, part_of_chunk)
        expand(0, lhs_even, part_of_chunk, part_of_chunk)

    parts = blocks // 2
    order = [first + part * subs for first in range(subs) for part in range(block_total // subs)]
    for turn, block in enumerate(order):
        following = order[turn + 1] if turn + 1 < block_total else block

        @pl.loop(0, chunks // 2)
        def _(couple):
            total = jnp.where(couple == 0, 0.0, acc[...])
            for parity in range(2):
                chunk = couple * 2 + parity
                wide = pl.ds(pl.multiple_of(chunk * (PIECES * CHUNK), LANES), PIECES * CHUNK)
                right = rhs[:, wide] if turn else rhs_sides[parity][...]
                total = total + dot_nt(lhs_sides[parity][...], right)
                coming = lax.rem(chunk + 1, chunks)
                coming_block = jnp.where(coming == 0, following, block)
                for part_of_chunk in range(2):
                    tile = coming * 2 + part_of_chunk
                    if turn == 0:
                        prepare(tile, rhs_sides[1 - parity], part_of_chunk)
                    expand(coming_block, lhs_sides[1 - parity], tile, part_of_chunk)
            acc[...] = total

        x_row = block * XBLOCK + lax.broadcasted_iota(jnp.int32, (XBLOCK, 1), 0)
        x_coord = (x_row - GRID // 2).astype(jnp.float32) * (field_of_view / GRID)
        depth = jnp.sqrt(1.0 - x_coord * x_coord - y_coord * y_coord) - 1.0
        above = jnp.zeros((XBLOCK, pixels), jnp.float32)
        below = jnp.zeros((XBLOCK, pixels), jnp.float32)
        for item in range(layer_dev):
            first = item * 2 * pixels
            p_ac = acc[:XBLOCK, first : first + pixels]
            p_ad = acc[:XBLOCK, first + pixels : first + 2 * pixels]
            p_bc = acc[XBLOCK:, first : first + pixels]
            p_bd = acc[XBLOCK:, first + pixels : first + 2 * pixels]
            cos_part, sin_part = turn_cos_sin(depth_ref[item] * depth)
            if block == 0:
                top = x_row == 0
                top_cos, top_sin = turn_cos_sin(depth_ref[item] * top_depth)
                top_value = p_bc * top_cos - p_bd * top_sin
                p_bc = jnp.where(top, 0.0, p_bc)
                p_bd = jnp.where(top, 0.0, p_bd)
            above += (p_ac - p_bd) * cos_part - (p_ad + p_bc) * sin_part
            lower = (p_ac + p_bd) * cos_part - (p_ad - p_bc) * sin_part
            if block == 0:
                lower = jnp.where(top, top_value, lower)
            below += lower
        part, sub = block // subs, block % subs
        rows = slice(sub * XBLOCK, (sub + 1) * XBLOCK)
        for owner, value in ((part, above), (blocks - 1 - part, below)):
            image[owner, rows, :] = value

            @pl.when(me_wa != owner)
            def _():
                image_copy(owner, sub).start()

        if sub == 0:
            target = blocks - 1 - (part - 1) % parts
            tail[target, 1:2, :] = below[0:1]

    tail_copies = [tail_copy(step) for step in range(1, blocks)]
    start_all(tail_copies)
    total = image[me_wa]
    total_tail = tail[me_wa]
    for step in range(1, blocks):
        for sub in range(subs):
            rows = pl.ds(sub * XBLOCK, XBLOCK)
            pltpu.make_async_remote_copy(
                src_ref=image.at[me_wa, rows],
                dst_ref=held.at[step - 1, rows],
                send_sem=image_send.at[me_wa, sub],
                recv_sem=image_recv.at[step - 1, sub],
                device_id={"wa": lax.rem(me_wa + step, blocks)},
                device_id_type=MESH,
            ).wait_recv()
        total = total + held[step - 1]
    for step, copy in enumerate(tail_copies):
        copy.wait()
        total_tail = total_tail + held_tail[step]
    scale = 1.0 / jnp.sqrt(total_tail[0:1])
    out_row = lax.broadcasted_iota(jnp.int32, (chunk_rows, chunk_rows), 0)
    in_row = lax.broadcasted_iota(jnp.int32, (chunk_rows, chunk_rows), 1)
    mirrored = me_wa * 2 >= blocks
    turned = jnp.where(mirrored, (chunk_rows - out_row) % chunk_rows, out_row)
    chosen = jnp.where(turned == in_row, 1.0, 0.0).astype(jnp.bfloat16)
    high, rest = split(total)
    low, last = split(total - high.astype(jnp.float32))
    ordered = sum(
        jnp.dot(chosen, piece, preferred_element_type=jnp.float32) for piece in (high, low, last)
    )
    out_line = lax.broadcasted_iota(jnp.int32, (chunk_rows, 1), 0)
    swap = jnp.where(mirrored, out_line, 1) == 0
    out_ref[...] = jnp.where(swap, total_tail[1:2], ordered) * scale
    for owner in range(blocks):

        @pl.when(me_wa != owner)
        def _():
            for sub in range(subs):
                image_copy(owner, sub).wait_send()


def body(
    visibilities,
    weights,
    cell_index,
    kernel_index,
    layer_index,
    tile_counts,
    kernel_table,
    layer_depth,
):
    layer_dev = layer_depth.shape[0]
    peers = lax.axis_size("bl")
    blocks = lax.axis_size("wa")
    pixels = GRID // peers
    chunk_rows = GRID // blocks
    own_tiles = cell_index.shape[1]
    tiles = peers * own_tiles
    count = tiles * LANES
    half = GRID // 2
    columns = 2 * layer_dev * pixels
    vmem = pl.BlockSpec(memory_space=pltpu.VMEM)
    smem = pl.BlockSpec(memory_space=pltpu.SMEM)
    f32, bf16 = jnp.float32, jnp.bfloat16
    shapes = [
        ((own_tiles, 8, LANES), f32),
        ((tiles, 8, LANES), f32),
        ((LANES, LANES), f32),
        ((half, LANES), f32),
        ((half, LANES), f32),
        ((pixels, LANES), f32),
        ((pixels, LANES), f32),
        ((FINE, count), f32),
        ((FINE, count), f32),
        ((half // XBLOCK, XBLOCK // FINE, count), f32),
        ((half // XBLOCK, XBLOCK // FINE, count), f32),
        ((columns, PIECES * count), bf16),
        ((2 * XBLOCK, PIECES * CHUNK), bf16),
        ((2 * XBLOCK, PIECES * CHUNK), bf16),
        ((columns, PIECES * CHUNK), bf16),
        ((columns, PIECES * CHUNK), bf16),
        ((2 * XBLOCK, columns), f32),
        ((blocks, chunk_rows, pixels), f32),
        ((blocks, 8, pixels), f32),
        ((blocks - 1, chunk_rows, pixels), f32),
        ((blocks - 1, 8, pixels), f32),
    ]
    subs = chunk_rows // XBLOCK
    semaphores = [
        (peers - 1,),
        (peers - 1,),
        (blocks, subs),
        (blocks - 1, subs),
        (blocks - 1,),
        (blocks - 1,),
    ]
    return pl.pallas_call(
        functools.partial(kernel, layer_dev, pixels, blocks, peers),
        out_shape=jax.ShapeDtypeStruct((chunk_rows, pixels), f32),
        in_specs=[smem, smem] + [vmem] * 6,
        out_specs=vmem,
        scratch_shapes=[pltpu.VMEM(shape, kind) for shape, kind in shapes]
        + [pltpu.SemaphoreType.DMA(shape) for shape in semaphores],
        compiler_params=pltpu.CompilerParams(
            collective_id=0, has_side_effects=True, vmem_limit_bytes=48 * 1024 * 1024
        ),
        name="dirty_image",
    )(
        layer_depth,
        tile_counts,
        kernel_table,
        visibilities,
        weights,
        cell_index,
        kernel_index,
        layer_index,
    )


def solution(mesh):
    in_specs = (
        P("wa", "bl", None, None),
        P("wa", "bl", None),
        P("wa", "bl", None),
        P("wa", "bl", None),
        P("wa", "bl", None),
        P("wa", "bl"),
        P(),
        P("wa"),
    )
    out_specs = P("wa", "bl")
    return jax.shard_map(body, mesh=mesh, in_specs=in_specs, out_specs=out_specs, check_vma=False)
```

```python
import functools
import math

import jax
import jax.numpy as jnp
from jax import lax
from jax.experimental import pallas as pl
from jax.experimental.pallas import tpu as pltpu
from jax.sharding import PartitionSpec as P

GRID = 1024
SUPPORT = 8
OVERSAMPLE = 16
LANES = 128
FINE = 32
XBLOCK = 128
CHUNK = 2 * LANES
PIECES = 3

field_of_view = 0.6
MESH = pl.DeviceIdType.MESH

TWO_PI = 2.0 * math.pi
SIN_TERMS = [(-1) ** k * TWO_PI ** (2 * k + 1) / math.factorial(2 * k + 1) for k in range(8)]
COS_TERMS = [(-1) ** k * TWO_PI ** (2 * k) / math.factorial(2 * k) for k in range(9)]


def horner(square, terms):
    value = jnp.full_like(square, terms[-1])
    for term in terms[-2::-1]:
        value = value * square + term
    return value


def turn_cos_sin(turns):
    part = turns - jnp.round(turns)
    square = part * part
    return horner(square, COS_TERMS), part * horner(square, SIN_TERMS)


def split(value):
    high = value.astype(jnp.bfloat16)
    return high, (value - high.astype(jnp.float32)).astype(jnp.bfloat16)


def dot_nt(a, b):
    return lax.dot_general(
        a, b, (((1,), (1,)), ((), ())), preferred_element_type=jnp.float32
    )


def factor_table(first, rows, table, special):
    pixel = (first + lax.broadcasted_iota(jnp.int32, (rows, LANES), 0)).astype(jnp.float32)
    offset_lane = lax.broadcasted_iota(jnp.int32, (rows, LANES), 1)
    offset = (offset_lane % SUPPORT - SUPPORT // 2).astype(jnp.float32)
    cos_part, sin_part = turn_cos_sin(pixel * offset * (1.0 / GRID))
    if special:
        row = lax.broadcasted_iota(jnp.int32, (rows, LANES), 0)
        parity = 1.0 - 2.0 * (offset_lane % 2).astype(jnp.float32)
        sin_part = jnp.where(row == 0, parity, sin_part)
    table_high, table_low = split(table)

    def product(part):
        high, low = split(part)
        return dot_nt(high, table_high) + dot_nt(high, table_low) + dot_nt(low, table_high)

    return product(cos_part), product(sin_part)


def start_all(copies):
    for copy in copies:
        copy.start()


def kernel(
    layer_dev,
    pixels,
    blocks,
    peers,
    depth_ref,
    counts_ref,
    table_ref,
    vis_ref,
    weight_ref,
    cell_ref,
    index_ref,
    layer_ref,
    out_ref,
    own,
    slots_ref,
    table_pad,
    phase_cos,
    phase_sin,
    u_re,
    u_im,
    v_re,
    v_im,
    fine_re,
    fine_im,
    coarse_re,
    coarse_im,
    rhs,
    lhs_even,
    lhs_odd,
    rhs_even,
    rhs_odd,
    acc,
    image,
    tail,
    held,
    held_tail,
    slot_send,
    slot_recv,
    image_send,
    image_recv,
    tail_send,
    tail_recv,
):
    half = GRID // 2
    chunk_rows = GRID // blocks
    own_tiles = own.shape[0]
    tiles = peers * own_tiles
    block_total = half // XBLOCK
    subs = chunk_rows // XBLOCK
    block_groups = XBLOCK // FINE
    me_bl, me_wa = lax.axis_index("bl"), lax.axis_index("wa")
    barrier = pltpu.get_barrier_semaphore()
    for axis, me, count in (("bl", me_bl, peers), ("wa", me_wa, blocks)):
        for step in range(1, count):
            pl.semaphore_signal(
                barrier, inc=1, device_id={axis: lax.rem(me + step, count)}, device_id_type=MESH
            )
    position = lax.broadcasted_iota(jnp.int32, (1, LANES), 1)
    for tile in range(own_tiles):
        line = slice(tile, tile + 1)
        weight = jnp.where(position < counts_ref[0, tile], weight_ref[0, line], 0.0)
        cell, index = cell_ref[0, line], index_ref[0, line]
        values = [
            vis_ref[0, tile, 0:1] * weight,
            vis_ref[0, tile, 1:2] * weight,
            weight,
            (cell // GRID).astype(jnp.float32),
            (cell % GRID).astype(jnp.float32),
            (index // OVERSAMPLE).astype(jnp.float32),
            (index % OVERSAMPLE).astype(jnp.float32),
            layer_ref[0, line].astype(jnp.float32),
        ]
        for place, value in enumerate(values):
            own[tile, place : place + 1] = value
    pl.semaphore_wait(barrier, peers + blocks - 2)
    slot_copies = [
        pltpu.make_async_remote_copy(
            src_ref=own,
            dst_ref=slots_ref.at[pl.ds(me_bl * own_tiles, own_tiles)],
            send_sem=slot_send.at[step - 1],
            recv_sem=slot_recv.at[step - 1],
            device_id={"bl": lax.rem(me_bl + step, peers)},
            device_id_type=MESH,
        )
        for step in range(1, peers)
    ]
    start_all(slot_copies)
    slots_ref[pl.ds(me_bl * own_tiles, own_tiles)] = own[...]

    first_pixel = me_bl * pixels
    table_pad[...] = jnp.zeros_like(table_pad)
    table_pad[0:OVERSAMPLE, 0:SUPPORT] = table_ref[...]
    table = table_pad[...]
    u_re[...], u_im[...] = factor_table(0, half, table, True)
    v_re[...], v_im[...] = factor_table(first_pixel, pixels, table, False)
    fine_x = lax.broadcasted_iota(jnp.int32, (FINE, LANES), 0).astype(jnp.float32)
    coarse_x = (lax.broadcasted_iota(jnp.int32, (half // FINE, LANES), 0) * FINE).astype(
        jnp.float32
    )
    pixel_y = (
        first_pixel + lax.broadcasted_iota(jnp.int32, (pixels // FINE, LANES), 0) * FINE
    ).astype(jnp.float32)
    y_pixel = first_pixel + lax.broadcasted_iota(jnp.int32, (1, pixels), 1)
    y_coord = (y_pixel - GRID // 2).astype(jnp.float32) * (field_of_view / GRID)
    top_depth = jnp.sqrt(1.0 - y_coord * y_coord) - 1.0
    for block in range(block_total):
        x_row = block * XBLOCK + lax.broadcasted_iota(jnp.int32, (XBLOCK, 1), 0)
        x_coord = (x_row - GRID // 2).astype(jnp.float32) * (field_of_view / GRID)
        depth = jnp.sqrt(1.0 - x_coord * x_coord - y_coord * y_coord) - 1.0
        lines = slice(block * XBLOCK, (block + 1) * XBLOCK)
        for item in range(layer_dev):
            cos_part, sin_part = turn_cos_sin(depth_ref[item] * depth)
            phase_cos[item, lines, :] = cos_part
            phase_sin[item, lines, :] = sin_part
    for copy in slot_copies:
        copy.wait()

    def lanes_of(tile):
        return pl.ds(pl.multiple_of(tile * LANES, LANES), LANES)

    def piece_lanes(tile):
        base = tile // 2 * (PIECES * CHUNK) + tile % 2 * LANES
        return [
            pl.ds(pl.multiple_of(base + piece * CHUNK, LANES), LANES) for piece in range(PIECES)
        ]

    def stage_lanes(part_of_chunk):
        starts = [piece * CHUNK + part_of_chunk * LANES for piece in range(PIECES)]
        return [slice(start, start + LANES) for start in starts]

    def prepare(tile, stage, part_of_chunk):
        lanes = lanes_of(tile)
        places = piece_lanes(tile)
        staged = stage_lanes(part_of_chunk)
        params = slots_ref[tile]
        vis_real, vis_imag = params[0:1], params[1:2]
        row, col = params[3:4] * (1.0 / GRID), params[4:5] * (1.0 / GRID)
        col_kernel = params[6:7].astype(jnp.int32)
        layer = params[7:8]
        fine_re[:, lanes], fine_im[:, lanes] = turn_cos_sin(row * fine_x)
        cx_re, cx_im = turn_cos_sin(row * coarse_x)
        for block in range(block_total):
            lines = slice(block * block_groups, (block + 1) * block_groups)
            coarse_re[block, :, lanes] = cx_re[lines]
            coarse_im[block, :, lanes] = cx_im[lines]
        cf_re, cf_im = turn_cos_sin(col * fine_x)
        cc_re, cc_im = turn_cos_sin(col * pixel_y)
        cv_re = cc_re * vis_real - cc_im * vis_imag
        cv_im = cc_re * vis_imag + cc_im * vis_real
        masks = [
            jnp.broadcast_to(jnp.where(layer == float(item), 1.0, 0.0), (FINE, LANES))
            for item in range(layer_dev)
        ]
        index = jnp.broadcast_to(col_kernel, (FINE, LANES))
        for group in range(pixels // FINE):
            rows = slice(group * FINE, (group + 1) * FINE)
            k_re = jnp.take_along_axis(v_re[rows, :], index, axis=1, mode="promise_in_bounds")
            k_im = jnp.take_along_axis(v_im[rows, :], index, axis=1, mode="promise_in_bounds")
            e_re = cf_re * cv_re[group : group + 1] - cf_im * cv_im[group : group + 1]
            e_im = cf_re * cv_im[group : group + 1] + cf_im * cv_re[group : group + 1]
            real = e_re * k_re - e_im * k_im
            imag = e_re * k_im + e_im * k_re
            for item in range(layer_dev):
                for place, value in enumerate((real, imag)):
                    high, low = split(value * masks[item])
                    start = (item * 2 + place) * pixels + group * FINE
                    for where, near, piece in zip(places, staged, (high, low, high)):
                        rhs[start : start + FINE, where] = piece
                        stage[start : start + FINE, near] = piece

    square_sum = jnp.sum(slots_ref[:, 2:3, :] * slots_ref[:, 2:3, :])

    def expand(block, side, tile, part_of_chunk):
        lanes = lanes_of(tile)
        places = stage_lanes(part_of_chunk)
        params = slots_ref[tile]
        index = jnp.broadcast_to(params[5:6].astype(jnp.int32), (FINE, LANES))
        f_re, f_im = fine_re[:, lanes], fine_im[:, lanes]
        c_re, c_im = coarse_re[block, :, lanes], coarse_im[block, :, lanes]
        for group in range(XBLOCK // FINE):
            place = block * (XBLOCK // FINE) + group
            rows = pl.ds(pl.multiple_of(place * FINE, FINE), FINE)
            k_re = jnp.take_along_axis(u_re[rows, :], index, axis=1, mode="promise_in_bounds")
            k_im = jnp.take_along_axis(u_im[rows, :], index, axis=1, mode="promise_in_bounds")
            g_re, g_im = c_re[group : group + 1], c_im[group : group + 1]
            e_re = f_re * g_re - f_im * g_im
            e_im = f_re * g_im + f_im * g_re
            real = e_re * k_re - e_im * k_im
            imag = e_re * k_im + e_im * k_re
            if group == 0:
                odd = params[3:4].astype(jnp.int32) % 2
                sign = (1 - 2 * odd).astype(jnp.float32)
                first_row = lax.broadcasted_iota(jnp.int32, (FINE, LANES), 0) == 0
                imag = imag * jnp.where(first_row & (block == 0), sign, 1.0)
            for part, value in enumerate((real, imag)):
                high, low = split(value)
                start = part * XBLOCK + group * FINE
                for where, piece in zip(places, (high, high, low)):
                    side[start : start + FINE, where] = piece

    def image_copy(owner, sub):
        slot = lax.rem(owner - me_wa + blocks, blocks) - 1
        rows = pl.ds(sub * XBLOCK, XBLOCK)
        return pltpu.make_async_remote_copy(
            src_ref=image.at[owner, rows],
            dst_ref=held.at[slot, rows],
            send_sem=image_send.at[owner, sub],
            recv_sem=image_recv.at[slot, sub],
            device_id={"wa": owner},
            device_id_type=MESH,
        )

    def tail_copy(step):
        peer = lax.rem(me_wa + step, blocks)
        return pltpu.make_async_remote_copy(
            src_ref=tail.at[peer],
            dst_ref=held_tail.at[step - 1],
            send_sem=tail_send.at[step - 1],
            recv_sem=tail_recv.at[step - 1],
            device_id={"wa": peer},
            device_id_type=MESH,
        )

    tail[...] = jnp.full_like(tail, square_sum)

    chunks = tiles // 2
    lhs_sides, rhs_sides = (lhs_even, lhs_odd), (rhs_even, rhs_odd)
    for part_of_chunk in range(2):
        prepare(part_of_chunk, rhs_even, part_of_chunk)
        expand(0, lhs_even, part_of_chunk, part_of_chunk)

    parts = blocks // 2
    order = [first + part * subs for first in range(subs) for part in range(block_total // subs)]
    for turn, block in enumerate(order):
        following = order[turn + 1] if turn + 1 < block_total else block

        @pl.loop(0, chunks // 2)
        def _(couple):
            total = jnp.where(couple == 0, 0.0, acc[...])
            for parity in range(2):
                chunk = couple * 2 + parity
                wide = pl.ds(pl.multiple_of(chunk * (PIECES * CHUNK), LANES), PIECES * CHUNK)
                right = rhs[:, wide] if turn else rhs_sides[parity][...]
                total = total + dot_nt(lhs_sides[parity][...], right)
                coming = lax.rem(chunk + 1, chunks)
                coming_block = jnp.where(coming == 0, following, block)
                for part_of_chunk in range(2):
                    tile = coming * 2 + part_of_chunk
                    if turn == 0:
                        prepare(tile, rhs_sides[1 - parity], part_of_chunk)
                    expand(coming_block, lhs_sides[1 - parity], tile, part_of_chunk)
            acc[...] = total

        x_row = block * XBLOCK + lax.broadcasted_iota(jnp.int32, (XBLOCK, 1), 0)
        lines = slice(block * XBLOCK, (block + 1) * XBLOCK)
        above = jnp.zeros((XBLOCK, pixels), jnp.float32)
        below = jnp.zeros((XBLOCK, pixels), jnp.float32)
        for item in range(layer_dev):
            first = item * 2 * pixels
            p_ac = acc[:XBLOCK, first : first + pixels]
            p_ad = acc[:XBLOCK, first + pixels : first + 2 * pixels]
            p_bc = acc[XBLOCK:, first : first + pixels]
            p_bd = acc[XBLOCK:, first + pixels : first + 2 * pixels]
            cos_part, sin_part = phase_cos[item, lines, :], phase_sin[item, lines, :]
            if block == 0:
                top = x_row == 0
                top_cos, top_sin = turn_cos_sin(depth_ref[item] * top_depth)
                top_value = p_bc * top_cos - p_bd * top_sin
                p_bc = jnp.where(top, 0.0, p_bc)
                p_bd = jnp.where(top, 0.0, p_bd)
            above += (p_ac - p_bd) * cos_part - (p_ad + p_bc) * sin_part
            lower = (p_ac + p_bd) * cos_part - (p_ad - p_bc) * sin_part
            if block == 0:
                lower = jnp.where(top, top_value, lower)
            below += lower
        part, sub = block // subs, block % subs
        rows = slice(sub * XBLOCK, (sub + 1) * XBLOCK)
        for owner, value in ((part, above), (blocks - 1 - part, below)):
            image[owner, rows, :] = value

            @pl.when(me_wa != owner)
            def _():
                image_copy(owner, sub).start()

        if sub == 0:
            target = blocks - 1 - (part - 1) % parts
            tail[target, 1:2, :] = below[0:1]

    tail_copies = [tail_copy(step) for step in range(1, blocks)]
    start_all(tail_copies)
    total = image[me_wa]
    total_tail = tail[me_wa]
    for step in range(1, blocks):
        for sub in range(subs):
            rows = pl.ds(sub * XBLOCK, XBLOCK)
            pltpu.make_async_remote_copy(
                src_ref=image.at[me_wa, rows],
                dst_ref=held.at[step - 1, rows],
                send_sem=image_send.at[me_wa, sub],
                recv_sem=image_recv.at[step - 1, sub],
                device_id={"wa": lax.rem(me_wa + step, blocks)},
                device_id_type=MESH,
            ).wait_recv()
        total = total + held[step - 1]
    for step, copy in enumerate(tail_copies):
        copy.wait()
        total_tail = total_tail + held_tail[step]
    scale = 1.0 / jnp.sqrt(total_tail[0:1])
    out_row = lax.broadcasted_iota(jnp.int32, (chunk_rows, chunk_rows), 0)
    in_row = lax.broadcasted_iota(jnp.int32, (chunk_rows, chunk_rows), 1)
    mirrored = me_wa * 2 >= blocks
    turned = jnp.where(mirrored, (chunk_rows - out_row) % chunk_rows, out_row)
    chosen = jnp.where(turned == in_row, 1.0, 0.0).astype(jnp.bfloat16)
    high, rest = split(total)
    low, last = split(total - high.astype(jnp.float32))
    ordered = sum(
        jnp.dot(chosen, piece, preferred_element_type=jnp.float32) for piece in (high, low, last)
    )
    out_line = lax.broadcasted_iota(jnp.int32, (chunk_rows, 1), 0)
    swap = jnp.where(mirrored, out_line, 1) == 0
    out_ref[...] = jnp.where(swap, total_tail[1:2], ordered) * scale
    for owner in range(blocks):

        @pl.when(me_wa != owner)
        def _():
            for sub in range(subs):
                image_copy(owner, sub).wait_send()


def body(
    visibilities,
    weights,
    cell_index,
    kernel_index,
    layer_index,
    tile_counts,
    kernel_table,
    layer_depth,
):
    layer_dev = layer_depth.shape[0]
    peers = lax.axis_size("bl")
    blocks = lax.axis_size("wa")
    pixels = GRID // peers
    chunk_rows = GRID // blocks
    own_tiles = cell_index.shape[1]
    tiles = peers * own_tiles
    count = tiles * LANES
    half = GRID // 2
    columns = 2 * layer_dev * pixels
    vmem = pl.BlockSpec(memory_space=pltpu.VMEM)
    smem = pl.BlockSpec(memory_space=pltpu.SMEM)
    f32, bf16 = jnp.float32, jnp.bfloat16
    shapes = [
        ((own_tiles, 8, LANES), f32),
        ((tiles, 8, LANES), f32),
        ((LANES, LANES), f32),
        ((layer_dev, half, pixels), f32),
        ((layer_dev, half, pixels), f32),
        ((half, LANES), f32),
        ((half, LANES), f32),
        ((pixels, LANES), f32),
        ((pixels, LANES), f32),
        ((FINE, count), f32),
        ((FINE, count), f32),
        ((half // XBLOCK, XBLOCK // FINE, count), f32),
        ((half // XBLOCK, XBLOCK // FINE, count), f32),
        ((columns, PIECES * count), bf16),
        ((2 * XBLOCK, PIECES * CHUNK), bf16),
        ((2 * XBLOCK, PIECES * CHUNK), bf16),
        ((columns, PIECES * CHUNK), bf16),
        ((columns, PIECES * CHUNK), bf16),
        ((2 * XBLOCK, columns), f32),
        ((blocks, chunk_rows, pixels), f32),
        ((blocks, 8, pixels), f32),
        ((blocks - 1, chunk_rows, pixels), f32),
        ((blocks - 1, 8, pixels), f32),
    ]
    subs = chunk_rows // XBLOCK
    semaphores = [
        (peers - 1,),
        (peers - 1,),
        (blocks, subs),
        (blocks - 1, subs),
        (blocks - 1,),
        (blocks - 1,),
    ]
    return pl.pallas_call(
        functools.partial(kernel, layer_dev, pixels, blocks, peers),
        out_shape=jax.ShapeDtypeStruct((chunk_rows, pixels), f32),
        in_specs=[smem, smem] + [vmem] * 6,
        out_specs=vmem,
        scratch_shapes=[pltpu.VMEM(shape, kind) for shape, kind in shapes]
        + [pltpu.SemaphoreType.DMA(shape) for shape in semaphores],
        compiler_params=pltpu.CompilerParams(
            collective_id=0, has_side_effects=True, vmem_limit_bytes=48 * 1024 * 1024
        ),
        name="dirty_image",
    )(
        layer_depth,
        tile_counts,
        kernel_table,
        visibilities,
        weights,
        cell_index,
        kernel_index,
        layer_index,
    )


def solution(mesh):
    in_specs = (
        P("wa", "bl", None, None),
        P("wa", "bl", None),
        P("wa", "bl", None),
        P("wa", "bl", None),
        P("wa", "bl", None),
        P("wa", "bl"),
        P(),
        P("wa"),
    )
    out_specs = P("wa", "bl")
    return jax.shard_map(body, mesh=mesh, in_specs=in_specs, out_specs=out_specs, check_vma=False)
```
